1024 devices in a mesh: gx: 64 (over x_hi, z, core), gy: 16 (over x_lo, y).
Axes of the slice: x: 4 (x_hi: 2, x_lo: 2; x = x_hi * 2 + x_lo), y: 8, z: 16, core: 2. Of those that a mesh axis runs over, the one named last changes fastest.
Arguments:
- velocity: float32 [3, 256, 128, 128], P(None, 'gx', 'gy'), may hold values from -4 to 4
- forcing: float32 [3, 256, 128, 128], P(None, 'gx', 'gy'), may hold values from -6 to 6
- viscosity: float32 [256, 128, 128], P('gx', 'gy'), may hold values from 0.05 to 0.5
- residual_prev: float32 [3, 256, 128, 128], P(None, 'gx', 'gy'), may hold values from -4 to 4
- value_prev: float32 [3, 256, 128, 128], P(None, 'gx', 'gy'), may hold values from -4 to 4
- hist_res: float32 [5, 3, 256, 128, 128], P(None, None, 'gx', 'gy'), may hold values from -16 to 16
- hist_val: float32 [5, 3, 256, 128, 128], P(None, None, 'gx', 'gy'), may hold values from -4 to 4
Outputs:
- velocity_out: float32 [3, 256, 128, 128], P(None, 'gx', 'gy')
- residual_out: float32 [3, 256, 128, 128], P(None, 'gx', 'gy')
The draws below stay inside these ranges and needn't reach their ends.
All inputs are finite; a program needn't handle non-finite values.
Results may differ from the reference program's by a relative error of at most 0.0003.
Values sent between devices are 32-bit elements; how exact they have to be, the bound alone decides.
No kernel may reach another device: no remote copies, remote signals or barrier semaphores. Data moves between devices by JAX's collectives and lax.ppermute only.
A program may use at most 64 MiB of HBM per device.

```python
import math
import jax
import jax.numpy as jnp
from jax import lax

CX = 4
CY = 8
NZ = 128
M = 5
SWEEPS = 3
ITERS = 2
NX = 256
NY = 128


def shared_forcing(key):
    base = jax.random.truncated_normal(jax.random.fold_in(key, 7), -5.0, 5.0, (3, NX, NY, NZ), jnp.float32)
    return base


def draw_forcing(key, part):
    return shared_forcing(key)


def draw_hist_res(key, part):
    forcing = shared_forcing(key)
    keys = jax.random.split(jax.random.fold_in(key, 11), 4)
    magnitude = jax.random.uniform(keys[0], (M,), jnp.float32, 0.4, 1.0)
    signs = jnp.where(jax.random.bernoulli(keys[1], 0.5, (M,)), 1.0, -1.0)
    coef = magnitude * signs
    blocks = jnp.exp(jax.random.uniform(keys[2], (M, 1, NX // CX, 1, NY // CY, 1, 1), jnp.float32, math.log(0.25), math.log(4.0)))
    noise = jax.random.truncated_normal(keys[3], -5.0, 5.0, (M, 3, NX, NY, NZ), jnp.float32)
    noise = (noise.reshape(M, 3, NX // CX, CX, NY // CY, CY, NZ) * blocks).reshape(M, 3, NX, NY, NZ)
    return coef[:, None, None, None, None] * forcing[None] + 0.5 * noise


def shard_levels(rng, extent, pieces, smallest, high):
    loudness = 1.0
    for dim, blocks in pieces:
        draws = jax.random.uniform(jax.random.fold_in(jax.random.fold_in(rng, 6), dim), (blocks,), jnp.float32, smallest / len(pieces), high / len(pieces))
        loudness = loudness * jnp.repeat(jnp.exp(draws), extent[dim] // blocks).reshape((-1,) + (1,) * (len(extent) - 1 - dim))
    return loudness


def centred(key, extent, deviation, limit, pieces=(), kind=jnp.bfloat16):
    result = jax.random.normal(key, extent, jnp.float32) * deviation
    if len(pieces) > 0:
        result = shard_levels(key, extent, pieces, -0.22, 0.18) * result
    return jnp.clip(result, min=-limit, max=limit).astype(kind)


def setup_inputs(seed: int = 0) -> dict:
    seeds = jax.random.split(jax.random.key(seed), 8)
    return {
        "velocity": centred(seeds[0], (3, NX, NY, NZ), 0.5, 4.0, ((1, 64), (2, 16)), jnp.float32),
        "forcing": draw_forcing(jax.random.fold_in(seeds[7], 71), 0),
        "viscosity": jnp.clip(jnp.exp(math.log(0.5) - 2.3025851 * jax.random.uniform(seeds[2], (NX, NY, NZ), jnp.float32) ** shard_levels(seeds[2], (NX, NY, NZ), ((0, 64), (1, 16)), -0.2, 0.2)), 0.05, 0.5),
        "residual_prev": centred(seeds[3], (3, NX, NY, NZ), 0.5, 4.0, ((1, 64), (2, 16)), jnp.float32),
        "value_prev": centred(seeds[4], (3, NX, NY, NZ), 0.5, 4.0, ((1, 64), (2, 16)), jnp.float32),
        "hist_res": draw_hist_res(jax.random.fold_in(seeds[7], 71), 0),
        "hist_val": centred(seeds[6], (M, 3, NX, NY, NZ), 0.5, 4.0, ((2, 64), (3, 16)), jnp.float32),
    }


REG = 0.05
FLOOR = 0.001

def relax(wide, vel, forcing, visc):
    deep = jnp.pad(wide, ((0, 0), (0, 0), (0, 0), (1, 1)))
    west = deep[:, :-2, 1:-1, 1:-1]
    east = deep[:, 2:, 1:-1, 1:-1]
    south = deep[:, 1:-1, :-2, 1:-1]
    north = deep[:, 1:-1, 2:, 1:-1]
    below = deep[:, 1:-1, 1:-1, :-2]
    above = deep[:, 1:-1, 1:-1, 2:]
    upward = jnp.maximum(vel, 0.0)
    downward = jnp.minimum(vel, 0.0)
    diag = 1.0 + 6.0 * visc + jnp.sum(jnp.abs(vel), axis=0)
    total = forcing + vel + visc * (west + east + south + north + below + above)
    total = total + upward[0] * west - downward[0] * east
    total = total + upward[1] * south - downward[1] * north
    total = total + upward[2] * below - downward[2] * above
    return total / diag

def picard(field, forcing, visc):
    state = field
    for sweep in range(SWEEPS):
        state = relax(jnp.pad(state, ((0, 0), (1, 1), (1, 1), (0, 0))), field, forcing, visc)
    return state

def reference(velocity, forcing, viscosity, residual_prev, value_prev, hist_res, hist_val):
    entries = 3.0 * NX * NY * NZ
    field = velocity
    res_last = residual_prev
    val_last = value_prev
    hist_f = hist_res
    hist_g = hist_val
    for step in range(ITERS):
        value = picard(field, forcing, viscosity)
        resid = value - field
        flat = hist_f.reshape(M, -1)
        gram = jnp.dot(flat, flat.T, precision=lax.Precision.HIGHEST)
        rhs = jnp.dot(flat, resid.reshape(-1), precision=lax.Precision.HIGHEST)
        shift = REG * jnp.trace(gram) / M + FLOOR * entries
        gamma = jnp.linalg.solve(gram + shift * jnp.eye(M, dtype=jnp.float32), rhs)
        field = value - jnp.tensordot(gamma, hist_g, axes=1, precision=lax.Precision.HIGHEST)
        hist_f = jnp.concatenate([hist_f[1:], (resid - res_last)[None]], 0)
        hist_g = jnp.concatenate([hist_g[1:], (value - val_last)[None]], 0)
        res_last = resid
        val_last = value
    return (field, res_last)
```

```python
import jax
import jax.numpy as jnp
from jax import lax
from jax.sharding import Mesh
from jax.sharding import PartitionSpec as P

M = 5
SWEEPS = 3
GX = ("gx_0", "gx_1", "gx_2")
GY = ("gy_0", "gy_1")
CHAIN = ("gx_1", "gx_2")
PLANE = ("gx_0", "gy_0", "gy_1")

REG = 0.05
FLOOR = 0.001
PAIRS = [(i, j) for i in range(M) for j in range(i, M)]


def padded(cells, sides, width):
    for axis, dim in sides:
        count = lax.axis_size(axis)
        ends = count - 1
        head = lax.slice_in_dim(cells, 0, width, axis=dim)
        tail = lax.slice_in_dim(cells, cells.shape[dim] - width, cells.shape[dim], axis=dim)
        cells = jnp.concatenate(
            [
                lax.ppermute(tail, axis, [(i, (i + 1) % count) for i in range(ends)]),
                cells,
                lax.ppermute(head, axis, [((i + 1) % count, i) for i in range(ends)]),
            ],
            axis=dim,
        )
    return cells


def total_over_devices(row):
    for group in (CHAIN, PLANE):
        count = lax.axis_size(group)
        rows = jnp.broadcast_to(row[None, None, :], (count, 1, row.shape[0]))
        row = jnp.sum(lax.all_to_all(rows, group, 0, 0), axis=(0, 1))
    return row


def relax(wide, vel, forcing, visc):
    deep = jnp.pad(wide, ((0, 0), (0, 0), (0, 0), (1, 1)))
    west = deep[:, :-2, 1:-1, 1:-1]
    east = deep[:, 2:, 1:-1, 1:-1]
    south = deep[:, 1:-1, :-2, 1:-1]
    north = deep[:, 1:-1, 2:, 1:-1]
    below = deep[:, 1:-1, 1:-1, :-2]
    above = deep[:, 1:-1, 1:-1, 2:]
    upward = jnp.maximum(vel, 0.0)
    downward = jnp.minimum(vel, 0.0)
    diag = 1.0 + 6.0 * visc + jnp.sum(jnp.abs(vel), axis=0)
    total = forcing + vel + visc * (west + east + south + north + below + above)
    total = total + upward[0] * west - downward[0] * east
    total = total + upward[1] * south - downward[1] * north
    total = total + upward[2] * below - downward[2] * above
    return total / diag


def picard(extended, static):
    state = extended
    for sweep in range(SWEEPS):
        edge = sweep + 1
        vel = extended[:, edge : extended.shape[1] - edge, edge : extended.shape[2] - edge]
        fixed = static[:, edge : static.shape[1] - edge, edge : static.shape[2] - edge]
        state = relax(state, vel, fixed[:3], fixed[3])
    return state


def solve_small(gram, rhs, entries):
    shift = REG * jnp.trace(gram) / M + FLOOR * entries
    factor = jnp.linalg.cholesky(gram + shift * jnp.eye(M, dtype=jnp.float32))
    return jax.scipy.linalg.cho_solve((factor, True), rhs)


def dot(a, b):
    return jnp.sum(a * b)


def mix(value, gamma, history):
    for j in range(M):
        value = value - gamma[j] * history[j]
    return value


def local(velocity, forcing, viscosity, residual_prev, value_prev, hist_res, hist_val):
    cells = velocity.shape[1] * velocity.shape[2] * velocity.shape[3]
    entries = 3.0 * cells * lax.axis_size(GX) * lax.axis_size(GY)
    sides = ((GX, 1), (GY, 2))
    both = padded(jnp.concatenate([velocity, forcing, viscosity[None]], 0), sides, SWEEPS)
    static = both[3:]

    value = picard(both[:3], static)
    resid = value - velocity
    newest = resid - residual_prev
    sums = [dot(hist_res[i], hist_res[j]) for i, j in PAIRS]
    sums += [dot(hist_res[i], resid) for i in range(M)]
    sums += [dot(hist_res[i], newest) for i in range(M)]
    sums += [dot(newest, newest)]
    sums = total_over_devices(jnp.pad(jnp.stack(sums), (0, 128 - len(sums))))
    first = len(PAIRS)
    place = {pair: k for k, pair in enumerate(PAIRS)}
    gram = jnp.stack(
        [sums[place[min(i, j), max(i, j)]] for i in range(M) for j in range(M)]
    ).reshape(M, M)
    gamma = solve_small(gram, sums[first : first + M], entries)
    field = mix(value, gamma, hist_val)

    cross = sums[first + M + 1 : first + 2 * M]
    gram_next = jnp.concatenate(
        [
            jnp.concatenate([gram[1:, 1:], cross[:, None]], 1),
            jnp.concatenate([cross, sums[first + 2 * M][None]])[None],
        ],
        0,
    )
    value_next = picard(padded(field, sides, SWEEPS), static)
    resid_next = value_next - field
    sums = [dot(hist_res[i], resid_next) for i in range(1, M)] + [dot(newest, resid_next)]
    sums = total_over_devices(jnp.pad(jnp.stack(sums), (0, 128 - M)))
    gamma = solve_small(gram_next, sums[:M], entries)
    field = mix(value_next, gamma, [*hist_val[1:], value - value_prev])
    return (field, resid_next)


def solution(mesh):
    torus = Mesh(mesh.devices.reshape(2, 16, 2, 2, 8), ("gx_0", "gx_1", "gx_2", "gy_0", "gy_1"))
    in_specs = (
        P(None, GX, GY, None),
        P(None, GX, GY, None),
        P(GX, GY, None),
        P(None, GX, GY, None),
        P(None, GX, GY, None),
        P(None, None, GX, GY, None),
        P(None, None, GX, GY, None),
    )
    out_specs = (P(None, GX, GY, None), P(None, GX, GY, None))
    return jax.shard_map(local, mesh=torus, in_specs=in_specs, out_specs=out_specs, check_vma=False)
```

```python
import jax
import jax.numpy as jnp
from jax import lax
from jax.experimental import pallas as pl
from jax.experimental.pallas import tpu as pltpu
from jax.sharding import Mesh
from jax.sharding import PartitionSpec as P

M = 5
SWEEPS = 3
AXES = ("gx_0", "gx_1", "gx_2", "gy_0", "gy_1")
GX = ("gx_0", "gx_1", "gx_2")
GY = ("gy_0", "gy_1")
CHAIN = ("gx_1", "gx_2")
PLANE = ("gx_0", "gy_0", "gy_1")

REG = 0.05
FLOOR = 0.001
PAIRS = [(i, j) for i in range(M) for j in range(i, M)]
RHS = len(PAIRS)
PREV = RHS + M
NORM = PREV + M

ROWS = 16
OWN = 3
FIELD = 3
STATIC = 4


def edge_rows(with_static):
    if with_static:
        return [(1, 3, 24, 0, False), (1, 4, 24, 24, True), (2, 8, 16, 48, True), (2, 6, 18, 64, False), (3, 9, 12, 88, False)], 104
    return [(1, 3, 24, 0, False), (2, 6, 18, 24, False), (3, 9, 12, 48, False)], 64


def call(kernel, outs, scratch=(), flops=20000):
    return pl.pallas_call(
        kernel,
        out_shape=[jax.ShapeDtypeStruct(s, jnp.float32) for s in outs],
        scratch_shapes=[pltpu.VMEM(s, jnp.float32) for s in scratch],
        compiler_params=pltpu.CompilerParams(vmem_limit_bytes=8 * 1024 * 1024),
        cost_estimate=pl.CostEstimate(flops=flops, bytes_accessed=100000, transcendentals=0),
    )


def pack_first(vel, forcing, visc, up, down):
    cx = vel.shape[1]
    for out, first_u, first_s in ((up, cx - 3, cx - 2), (down, 0, 0)):
        for d in range(3):
            for c in range(3):
                out[d * 3 + c] = vel[c, first_u + d]
        for d in range(2):
            for c in range(3):
                out[9 + d * 4 + c] = forcing[c, first_s + d]
            out[9 + d * 4 + 3] = visc[first_s + d]


def field_tile(vel, left, right, tile):
    plane, c = divmod(tile, FIELD)
    cx = vel.shape[1]
    if plane < 3:
        return left[tile]
    if plane < 3 + cx:
        return vel[c, plane - 3]
    return right[tile - (3 + cx) * FIELD]


def static_tile(forcing, visc, left, right, tile):
    plane, c = divmod(tile, STATIC)
    cx = visc.shape[0]
    if plane < 2:
        return left[9 + tile]
    if plane < 2 + cx:
        return forcing[c, plane - 2] if c < 3 else visc[plane - 2]
    return right[9 + tile - (2 + cx) * STATIC]


def pack_second(with_static, *refs):
    if with_static:
        vel, forcing, visc, left, right, up, down, tiles, fixed = refs
        for t in range(8 * STATIC):
            fixed[t * 8 : t * 8 + 8] = static_tile(forcing, visc, left, right, t)
    else:
        vel, left, right, up, down, tiles = refs
        fixed = None
    for t in range(10 * FIELD):
        tiles[t * 8 : t * 8 + 8] = field_tile(vel, left, right, t)
    pieces, _ = edge_rows(with_static)
    for dist, first, count, row, static in pieces:
        src = fixed if static else tiles
        up[row : row + count] = src[pl.ds(first * 8 + 8 - dist, count, stride=8), :]
        down[row : row + count] = src[pl.ds(first * 8 + dist - 1, count, stride=8), :]


def fill_frames(with_static, south, north, frames, fixed):
    pieces, _ = edge_rows(with_static)
    for dist, first, count, row, static in pieces:
        dst = fixed if static else frames
        dst[pl.ds(first * ROWS + OWN - dist, count, stride=ROWS), :] = south[row : row + count]
        dst[pl.ds(first * ROWS + OWN + 7 + dist, count, stride=ROWS), :] = north[row : row + count]


def sweeps(frames, fixed, coef, one, two):
    lane = lax.broadcasted_iota(jnp.int32, (ROWS, 128), 1)
    field = lambda p, c: frames[(p * FIELD + c) * ROWS : (p * FIELD + c + 1) * ROWS]
    still = lambda s, c: fixed[(s * STATIC + c) * ROWS : (s * STATIC + c + 1) * ROWS]
    for s in range(8):
        a = [field(s + 1, c) for c in range(3)]
        visc = still(s, 3)
        inv = 1.0 / (1.0 + 6.0 * visc + jnp.abs(a[0]) + jnp.abs(a[1]) + jnp.abs(a[2]))
        for k in range(3):
            low = (visc + jnp.maximum(a[k], 0.0)) * inv
            high = (visc - jnp.minimum(a[k], 0.0)) * inv
            if k == 2:
                low = jnp.where(lane > 0, low, 0.0)
                high = jnp.where(lane < 127, high, 0.0)
            coef[s, 2 * k] = low
            coef[s, 2 * k + 1] = high
            coef[s, 6 + k] = (still(s, k) + a[k]) * inv

    def relax(src, s, c):
        mid = src(0)
        total = coef[s, 6 + c] + coef[s, 0] * src(-1) + coef[s, 1] * src(1)
        total = total + coef[s, 2] * pltpu.roll(mid, 1, 0) + coef[s, 3] * pltpu.roll(mid, ROWS - 1, 0)
        return total + coef[s, 4] * pltpu.roll(mid, 1, 1) + coef[s, 5] * pltpu.roll(mid, 127, 1)

    for s in range(8):
        for c in range(3):
            one[s, c] = relax(lambda d: field(s + 1 + d, c), s, c)
    for s in range(1, 7):
        for c in range(3):
            two[s, c] = relax(lambda d: one[s + d, c], s, c)
    out = {}
    for s in range(2, 6):
        for c in range(3):
            out[c, s - 2] = relax(lambda d: two[s + d, c], s, c)[OWN : OWN + 8]
    return out


def lanes(row, shape=(1, 128)):
    return lax.broadcasted_iota(jnp.int32, shape, 1)


def spread(row, parts):
    lane = lanes(row)
    for k, part in parts.items():
        whole = jnp.sum(jnp.sum(part, axis=0, keepdims=True), axis=1, keepdims=True)
        row = jnp.where(lane == k, whole, row)
    return row


def gram_part(hist, prev, out):
    tiles = [(c, p) for c in range(3) for p in range(hist.shape[2])]
    parts = {}
    for k, (i, j) in enumerate(PAIRS):
        parts[k] = sum(hist[i, c, p] * hist[j, c, p] for c, p in tiles)
    for i in range(M):
        parts[PREV + i] = sum(hist[i, c, p] * prev[c, p] for c, p in tiles)
    out[...] = spread(jnp.zeros((1, 128), jnp.float32), parts)


def first_map(vel, forcing, visc, left, right, south, north, hist, prev, gram, value, newest, fixed, payload, frames, coef, one, two):
    frames[...] = jnp.zeros_like(frames)
    fixed[...] = jnp.zeros_like(fixed)
    for t in range(8 * STATIC):
        fixed[t * ROWS + OWN : t * ROWS + OWN + 8] = static_tile(forcing, visc, left, right, t)
    for t in range(10 * FIELD):
        frames[t * ROWS + OWN : t * ROWS + OWN + 8] = field_tile(vel, left, right, t)
    fill_frames(True, south, north, frames, fixed)
    result = sweeps(frames, fixed, coef, one, two)
    resid = {}
    fresh = {}
    for (c, p), tile in result.items():
        value[c, p] = tile
        resid[c, p] = tile - vel[c, p]
        fresh[c, p] = resid[c, p] - prev[c, p]
        newest[c, p] = fresh[c, p]
    parts = {RHS + i: sum(hist[i, c, p] * r for (c, p), r in resid.items()) for i in range(M)}
    parts[NORM] = sum(f * f for f in fresh.values())
    row = spread(gram[...], parts)
    for k in range(payload.shape[0]):
        payload[k] = row


def second_map(vel, left, right, south, north, fixed, hist, newest, value, resid, payload, frames, coef, one, two):
    frames[...] = jnp.zeros_like(frames)
    for t in range(10 * FIELD):
        frames[t * ROWS + OWN : t * ROWS + OWN + 8] = field_tile(vel, left, right, t)
    fill_frames(False, south, north, frames, None)
    result = sweeps(frames, fixed, coef, one, two)
    for (c, p), tile in result.items():
        value[c, p] = tile
        result[c, p] = tile - vel[c, p]
        resid[c, p] = result[c, p]
    parts = {i: sum(hist[i + 1, c, p] * r for (c, p), r in result.items()) for i in range(M - 1)}
    parts[M - 1] = sum(newest[c, p] * r for (c, p), r in result.items())
    row = spread(jnp.zeros((1, 128), jnp.float32), parts)
    for k in range(payload.shape[0]):
        payload[k] = row


def entry(row, k):
    return jnp.sum(jnp.where(lanes(row) == k, row, 0.0), axis=1, keepdims=True)


def solve(gram, rhs, entries):
    shift = (REG / M) * sum(gram[i, i] for i in range(M)) + FLOOR * entries
    a = {(i, j): gram[min(i, j), max(i, j)] for i in range(M) for j in range(M)}
    for i in range(M):
        a[i, i] = a[i, i] + shift
    r = list(rhs)
    inv = []
    for k in range(M):
        inv.append(1.0 / a[k, k])
        for i in range(k + 1, M):
            f = a[k, i] * inv[k]
            for j in range(i, M):
                a[i, j] = a[i, j] - f * a[k, j]
            r[i] = r[i] - f * r[k]
    out = [None] * M
    for i in reversed(range(M)):
        acc = r[i]
        for j in range(i + 1, M):
            acc = acc - a[i, j] * out[j]
        out[i] = acc * inv[i]
    return out


def gathered(rows):
    total = rows[0]
    for k in range(1, rows.shape[0]):
        total = total + rows[k]
    return total


def mix_first(entries, rows, value, hist, field, up, down):
    row = gathered(rows)
    s = [entry(row, k) for k in range(PREV)]
    gram = {pair: s[k] for k, pair in enumerate(PAIRS)}
    gamma = [jnp.broadcast_to(g, (8, 128)) for g in solve(gram, s[RHS:PREV], entries)]
    cx = value.shape[1]
    for c in range(3):
        for p in range(cx):
            tile = value[c, p]
            for j in range(M):
                tile = tile - gamma[j] * hist[j, c, p]
            field[c, p] = tile
            if p >= cx - 3:
                up[(p - cx + 3) * 3 + c] = tile
            if p < 3:
                down[p * 3 + c] = tile


def mix_second(entries, rows, first_rows, value, hist, first_value, prev, field):
    row = gathered(first_rows)
    s = [entry(row, k) for k in range(NORM + 1)]
    gram = {}
    for k, (i, j) in enumerate(PAIRS):
        if i > 0:
            gram[i - 1, j - 1] = s[k]
    for i in range(M - 1):
        gram[i, M - 1] = s[RHS + 1 + i] - s[PREV + 1 + i]
    gram[M - 1, M - 1] = s[NORM]
    row = gathered(rows)
    gamma = solve(gram, [entry(row, k) for k in range(M)], entries)
    gamma = [jnp.broadcast_to(g, (8, 128)) for g in gamma]
    for c in range(3):
        for p in range(value.shape[1]):
            tile = value[c, p]
            for j in range(M - 1):
                tile = tile - gamma[j] * hist[j + 1, c, p]
            field[c, p] = tile - gamma[M - 1] * (first_value[c, p] - prev[c, p])


def neighbours(axis, up, down):
    count = lax.axis_size(axis)
    ends = count - 1
    before = lax.ppermute(up, axis, [(i, i + 1) for i in range(ends)])
    after = lax.ppermute(down, axis, [(i + 1, i) for i in range(ends)])
    return before, after


def exchange(payload):
    row = jnp.sum(lax.all_to_all(payload, CHAIN, 0, 0), axis=(0, 1))
    rows = jnp.broadcast_to(row[None, None, :], (lax.axis_size(PLANE), 1, 128))
    return lax.all_to_all(rows, PLANE, 0, 0)


def local(velocity, forcing, viscosity, residual_prev, value_prev, hist_res, hist_val):
    shape = velocity.shape
    entries = 1.0 * velocity.size * lax.axis_size(GX) * lax.axis_size(GY)
    fan = (lax.axis_size(CHAIN), 1, 128)
    work = ((8, 9, ROWS, 128), (8, 3, ROWS, 128), (8, 3, ROWS, 128))
    frames = (10 * FIELD * ROWS, 128)
    fixed = (8 * STATIC * ROWS, 128)

    up, down = call(pack_first, [(17, 8, 128)] * 2)(velocity, forcing, viscosity)
    left, right = neighbours(GX, up, down)
    (gram,) = call(gram_part, [(1, 128)], flops=4000000)(hist_res, residual_prev)
    edge = (edge_rows(True)[1], 128)
    up, down = call(
        lambda *refs: pack_second(True, *refs), [edge, edge], [(10 * FIELD * 8, 128), (8 * STATIC * 8, 128)]
    )(velocity, forcing, viscosity, left, right)
    south, north = neighbours(GY, up, down)
    value, newest, static, payload = call(first_map, [shape, shape, fixed, fan], [frames, *work])(
        velocity, forcing, viscosity, left, right, south, north, hist_res, residual_prev, gram
    )
    sums = exchange(payload)
    field, up, down = call(lambda *refs: mix_first(entries, *refs), [shape, (9, 8, 128), (9, 8, 128)])(
        sums, value, hist_val
    )
    left, right = neighbours(GX, up, down)
    edge = (edge_rows(False)[1], 128)
    up, down = call(lambda *refs: pack_second(False, *refs), [edge, edge], [(10 * FIELD * 8, 128)])(
        field, left, right
    )
    south, north = neighbours(GY, up, down)
    value_next, resid, payload = call(second_map, [shape, shape, fan], [frames, *work])(
        field, left, right, south, north, static, hist_res, newest
    )
    (out,) = call(lambda *refs: mix_second(entries, *refs), [shape])(
        exchange(payload), sums, value_next, hist_val, value, value_prev
    )
    return (out, resid)


def build(torus):
    in_specs = (
        P(None, GX, GY, None),
        P(None, GX, GY, None),
        P(GX, GY, None),
        P(None, GX, GY, None),
        P(None, GX, GY, None),
        P(None, None, GX, GY, None),
        P(None, None, GX, GY, None),
    )
    out_specs = (P(None, GX, GY, None), P(None, GX, GY, None))
    return jax.shard_map(local, mesh=torus, in_specs=in_specs, out_specs=out_specs, check_vma=False)


def solution(mesh):
    return build(Mesh(mesh.devices.reshape(2, 16, 2, 2, 8), AXES))
```

```python
import jax
import jax.numpy as jnp
from jax import lax
from jax.experimental import pallas as pl
from jax.experimental.pallas import tpu as pltpu
from jax.sharding import Mesh
from jax.sharding import PartitionSpec as P

M = 5
SWEEPS = 3
AXES = ("gx_0", "gx_1", "gx_2", "gy_0", "gy_1")
GX = ("gx_0", "gx_1", "gx_2")
GY = ("gy_0", "gy_1")
CHAIN = ("gx_1", "gx_2")
PLANE = ("gx_0", "gy_0", "gy_1")

REG = 0.05
FLOOR = 0.001
PAIRS = [(i, j) for i in range(M) for j in range(i, M)]
RHS = len(PAIRS)
PREV = RHS + M
NORM = PREV + M

ROWS = 16
OWN = 3
FIELD = 3
STATIC = 4


def edge_rows(with_static):
    if with_static:
        return [(1, 3, 24, 0, False), (1, 4, 24, 24, True), (2, 8, 16, 48, True), (2, 6, 18, 64, False), (3, 9, 12, 88, False)], 104
    return [(1, 3, 24, 0, False), (2, 6, 18, 24, False), (3, 9, 12, 48, False)], 64


def call(kernel, outs, scratch=(), flops=20000, **more):
    return pl.pallas_call(
        kernel,
        out_shape=[jax.ShapeDtypeStruct(s, jnp.float32) for s in outs],
        scratch_shapes=[pltpu.VMEM(s, jnp.float32) if isinstance(s, tuple) else s for s in scratch],
        compiler_params=pltpu.CompilerParams(vmem_limit_bytes=8 * 1024 * 1024),
        cost_estimate=pl.CostEstimate(flops=flops, bytes_accessed=100000, transcendentals=0),
        **more,
    )


def place(axes):
    index = 0
    count = 1
    for axis in axes:
        index = index * lax.axis_size(axis) + lax.axis_index(axis)
        count = count * lax.axis_size(axis)
    return lax.rem(index, 2) == 1, index == 0, index == count - 1


def pack_first(vel, forcing, visc, even_pair, odd_pair, vel_near, forcing_near, visc_near, sem):
    cx = vel.shape[1]
    odd, _, _ = place(GX)
    copies = []
    for out, low in ((even_pair, odd), (odd_pair, jnp.logical_not(odd))):
        three = pl.ds(jnp.where(low, 0, cx - 3), 3)
        two = pl.ds(jnp.where(low, 0, cx - 2), 2)
        pieces = [(vel.at[c, three], out.at[pl.ds(3 * c, 3)]) for c in range(3)]
        pieces += [(forcing.at[c, two], out.at[pl.ds(9 + 2 * c, 2)]) for c in range(3)]
        pieces += [(visc.at[two], out.at[pl.ds(15, 2)])]
        for src, dst in pieces:
            copies.append(pltpu.make_async_copy(src, dst, sem.at[len(copies)]))
            copies[-1].start()
    for src, dst in ((vel, vel_near), (forcing, forcing_near), (visc, visc_near)):
        copies.append(pltpu.make_async_copy(src, dst, sem.at[len(copies)]))
        copies[-1].start()
    for copy in copies:
        copy.wait()


def arrived(axes, even_pair, odd_pair):
    odd, first, last = place(axes)
    before = lambda i: jnp.where(odd, even_pair[0, i], jnp.where(first, 0.0, odd_pair[0, i]))
    after = lambda i: jnp.where(odd, jnp.where(last, 0.0, odd_pair[1, i]), even_pair[1, i])
    return before, after


def field_tile(vel, left, right, tile):
    plane, c = divmod(tile, FIELD)
    cx = vel.shape[1]
    if plane < 3:
        return left(3 * c + plane)
    if plane < 3 + cx:
        return vel[c, plane - 3]
    return right(3 * c + plane - 3 - cx)


def static_tile(forcing, visc, left, right, tile):
    plane, c = divmod(tile, STATIC)
    cx = visc.shape[0]
    if plane < 2:
        return left(9 + 2 * c + plane)
    if plane < 2 + cx:
        return forcing[c, plane - 2] if c < 3 else visc[plane - 2]
    return right(9 + 2 * c + plane - 2 - cx)


def pack_second(with_static, *refs):
    if with_static:
        vel, forcing, visc, near, far, even_pair, odd_pair, tiles, fixed = refs
    else:
        vel, near, far, even_pair, odd_pair, tiles = refs
        fixed = None
    left, right = arrived(GX, near, far)
    if with_static:
        for t in range(8 * STATIC):
            fixed[t * 8 : t * 8 + 8] = static_tile(forcing, visc, left, right, t)
    for t in range(10 * FIELD):
        tiles[t * 8 : t * 8 + 8] = field_tile(vel, left, right, t)
    odd, _, _ = place(GY)
    pieces, _ = edge_rows(with_static)
    for dist, first, count, row, static in pieces:
        src = fixed if static else tiles
        up = src[pl.ds(first * 8 + 8 - dist, count, stride=8), :]
        down = src[pl.ds(first * 8 + dist - 1, count, stride=8), :]
        even_pair[row : row + count] = jnp.where(odd, down, up)
        odd_pair[row : row + count] = jnp.where(odd, up, down)


def fill_frames(with_static, even_pair, odd_pair, frames, fixed):
    pieces, _ = edge_rows(with_static)
    south, north = arrived(GY, even_pair, odd_pair)
    for dist, first, count, row, static in pieces:
        dst = fixed if static else frames
        dst[pl.ds(first * ROWS + OWN - dist, count, stride=ROWS), :] = south(pl.ds(row, count))
        dst[pl.ds(first * ROWS + OWN + 7 + dist, count, stride=ROWS), :] = north(pl.ds(row, count))


def sweeps(frames, fixed, coef, one, two):
    lane = lax.broadcasted_iota(jnp.int32, (ROWS, 128), 1)
    field = lambda p, c: frames[(p * FIELD + c) * ROWS : (p * FIELD + c + 1) * ROWS]
    still = lambda s, c: fixed[(s * STATIC + c) * ROWS : (s * STATIC + c + 1) * ROWS]
    for s in range(8):
        a = [field(s + 1, c) for c in range(3)]
        visc = still(s, 3)
        inv = 1.0 / (1.0 + 6.0 * visc + jnp.abs(a[0]) + jnp.abs(a[1]) + jnp.abs(a[2]))
        for k in range(3):
            low = (visc + jnp.maximum(a[k], 0.0)) * inv
            high = (visc - jnp.minimum(a[k], 0.0)) * inv
            if k == 2:
                low = jnp.where(lane > 0, low, 0.0)
                high = jnp.where(lane < 127, high, 0.0)
            coef[s, 2 * k] = low
            coef[s, 2 * k + 1] = high
            coef[s, 6 + k] = (still(s, k) + a[k]) * inv

    def relax(src, s, c):
        mid = src(0)
        total = coef[s, 6 + c] + coef[s, 0] * src(-1) + coef[s, 1] * src(1)
        total = total + coef[s, 2] * pltpu.roll(mid, 1, 0) + coef[s, 3] * pltpu.roll(mid, ROWS - 1, 0)
        return total + coef[s, 4] * pltpu.roll(mid, 1, 1) + coef[s, 5] * pltpu.roll(mid, 127, 1)

    for s in range(8):
        for c in range(3):
            one[s, c] = relax(lambda d: field(s + 1 + d, c), s, c)
    for s in range(1, 7):
        for c in range(3):
            two[s, c] = relax(lambda d: one[s + d, c], s, c)
    out = {}
    for s in range(2, 6):
        for c in range(3):
            out[c, s - 2] = relax(lambda d: two[s + d, c], s, c)[OWN : OWN + 8]
    return out


def lanes(row, shape=(1, 128)):
    return lax.broadcasted_iota(jnp.int32, shape, 1)


def spread(row, parts):
    lane = lanes(row)
    for k, part in parts.items():
        whole = jnp.sum(jnp.sum(part, axis=0, keepdims=True), axis=1, keepdims=True)
        row = jnp.where(lane == k, whole, row)
    return row


def gram_part(hist, prev, out):
    tiles = [(c, p) for c in range(3) for p in range(hist.shape[2])]
    parts = {}
    for k, (i, j) in enumerate(PAIRS):
        parts[k] = sum(hist[i, c, p] * hist[j, c, p] for c, p in tiles)
    for i in range(M):
        parts[PREV + i] = sum(hist[i, c, p] * prev[c, p] for c, p in tiles)
    out[...] = spread(jnp.zeros((1, 128), jnp.float32), parts)


def first_map(vel, forcing, visc, near, far, even_pair, odd_pair, hist, prev, gram, value, newest, fixed, payload, frames, coef, one, two):
    frames[...] = jnp.zeros_like(frames)
    fixed[...] = jnp.zeros_like(fixed)
    left, right = arrived(GX, near, far)
    for t in range(8 * STATIC):
        fixed[t * ROWS + OWN : t * ROWS + OWN + 8] = static_tile(forcing, visc, left, right, t)
    for t in range(10 * FIELD):
        frames[t * ROWS + OWN : t * ROWS + OWN + 8] = field_tile(vel, left, right, t)
    fill_frames(True, even_pair, odd_pair, frames, fixed)
    result = sweeps(frames, fixed, coef, one, two)
    resid = {}
    fresh = {}
    for (c, p), tile in result.items():
        value[c, p] = tile
        resid[c, p] = tile - vel[c, p]
        fresh[c, p] = resid[c, p] - prev[c, p]
        newest[c, p] = fresh[c, p]
    parts = {RHS + i: sum(hist[i, c, p] * r for (c, p), r in resid.items()) for i in range(M)}
    parts[NORM] = sum(f * f for f in fresh.values())
    row = spread(gram[...], parts)
    for k in range(payload.shape[0]):
        payload[k] = row


def second_map(vel, near, far, even_pair, odd_pair, fixed, hist, newest, value, resid, payload, frames, coef, one, two):
    frames[...] = jnp.zeros_like(frames)
    left, right = arrived(GX, near, far)
    for t in range(10 * FIELD):
        frames[t * ROWS + OWN : t * ROWS + OWN + 8] = field_tile(vel, left, right, t)
    fill_frames(False, even_pair, odd_pair, frames, None)
    result = sweeps(frames, fixed, coef, one, two)
    for (c, p), tile in result.items():
        value[c, p] = tile
        result[c, p] = tile - vel[c, p]
        resid[c, p] = result[c, p]
    parts = {i: sum(hist[i + 1, c, p] * r for (c, p), r in result.items()) for i in range(M - 1)}
    parts[M - 1] = sum(newest[c, p] * r for (c, p), r in result.items())
    row = spread(jnp.zeros((1, 128), jnp.float32), parts)
    for k in range(payload.shape[0]):
        payload[k] = row


def entry(row, k):
    return jnp.sum(jnp.where(lanes(row) == k, row, 0.0), axis=1, keepdims=True)


def solve(gram, rhs, entries):
    shift = (REG / M) * sum(gram[i, i] for i in range(M)) + FLOOR * entries
    a = {(i, j): gram[min(i, j), max(i, j)] for i in range(M) for j in range(M)}
    for i in range(M):
        a[i, i] = a[i, i] + shift
    r = list(rhs)
    inv = []
    for k in range(M):
        inv.append(1.0 / a[k, k])
        for i in range(k + 1, M):
            f = a[k, i] * inv[k]
            for j in range(i, M):
                a[i, j] = a[i, j] - f * a[k, j]
            r[i] = r[i] - f * r[k]
    out = [None] * M
    for i in reversed(range(M)):
        acc = r[i]
        for j in range(i + 1, M):
            acc = acc - a[i, j] * out[j]
        out[i] = acc * inv[i]
    return out


def gathered(rows):
    total = rows[0]
    for k in range(1, rows.shape[0]):
        total = total + rows[k]
    return total


def mix_first(entries, rows, value, hist, field, even_pair, odd_pair):
    row = gathered(rows)
    s = [entry(row, k) for k in range(PREV)]
    gram = {pair: s[k] for k, pair in enumerate(PAIRS)}
    gamma = [jnp.broadcast_to(g, (8, 128)) for g in solve(gram, s[RHS:PREV], entries)]
    cx = value.shape[1]
    odd, _, _ = place(GX)
    for c in range(3):
        mixed = []
        for p in range(cx):
            tile = value[c, p]
            for j in range(M):
                tile = tile - gamma[j] * hist[j, c, p]
            field[c, p] = tile
            mixed.append(tile)
        for d in range(3):
            even_pair[3 * c + d] = jnp.where(odd, mixed[d], mixed[cx - 3 + d])
            odd_pair[3 * c + d] = jnp.where(odd, mixed[cx - 3 + d], mixed[d])


def mix_second(entries, rows, first_rows, value, hist, first_value, prev, field):
    row = gathered(first_rows)
    s = [entry(row, k) for k in range(NORM + 1)]
    gram = {}
    for k, (i, j) in enumerate(PAIRS):
        if i > 0:
            gram[i - 1, j - 1] = s[k]
    for i in range(M - 1):
        gram[i, M - 1] = s[RHS + 1 + i] - s[PREV + 1 + i]
    gram[M - 1, M - 1] = s[NORM]
    row = gathered(rows)
    gamma = solve(gram, [entry(row, k) for k in range(M)], entries)
    gamma = [jnp.broadcast_to(g, (8, 128)) for g in gamma]
    for c in range(3):
        for p in range(value.shape[1]):
            tile = value[c, p]
            for j in range(M - 1):
                tile = tile - gamma[j] * hist[j + 1, c, p]
            field[c, p] = tile - gamma[M - 1] * (first_value[c, p] - prev[c, p])


def neighbours(axes, even_pair, odd_pair):
    count = lax.axis_size(axes)
    pairs = [[[i, (i + 1) % count] for i in range(start, count, 2)] for start in (0, 1)]
    return (
        lax.all_gather(even_pair, axes, axis_index_groups=pairs[0]),
        lax.all_gather(odd_pair, axes, axis_index_groups=pairs[1]),
    )


def exchange(payload):
    row = jnp.sum(lax.all_to_all(payload, CHAIN, 0, 0), axis=(0, 1))
    rows = jnp.broadcast_to(row[None, None, :], (lax.axis_size(PLANE), 1, 128))
    return lax.all_to_all(rows, PLANE, 0, 0)


def local(velocity, forcing, viscosity, residual_prev, value_prev, hist_res, hist_val):
    shape = velocity.shape
    entries = 1.0 * velocity.size * lax.axis_size(GX) * lax.axis_size(GY)
    fan = (lax.axis_size(CHAIN), 1, 128)
    work = ((8, 9, ROWS, 128), (8, 3, ROWS, 128), (8, 3, ROWS, 128))
    frames = (10 * FIELD * ROWS, 128)
    fixed = (8 * STATIC * ROWS, 128)

    hbm = [pl.BlockSpec(memory_space=pltpu.HBM)] * 3
    far_away = [pltpu.with_memory_space_constraint(x, pltpu.HBM) for x in (velocity, forcing, viscosity)]
    *packed, velocity, forcing, viscosity = call(
        pack_first, [(17, 8, 128)] * 2 + [shape, shape, shape[1:]], [pltpu.SemaphoreType.DMA((17,))], in_specs=hbm
    )(*far_away)
    faces = neighbours(GX, *packed)
    (gram,) = call(gram_part, [(1, 128)], flops=4000000)(hist_res, residual_prev)
    edge = (edge_rows(True)[1], 128)
    packed = call(
        lambda *refs: pack_second(True, *refs), [edge, edge], [(10 * FIELD * 8, 128), (8 * STATIC * 8, 128)]
    )(velocity, forcing, viscosity, *faces)
    edges = neighbours(GY, *packed)
    value, newest, static, payload = call(first_map, [shape, shape, fixed, fan], [frames, *work])(
        velocity, forcing, viscosity, *faces, *edges, hist_res, residual_prev, gram
    )
    sums = exchange(payload)
    field, *packed = call(lambda *refs: mix_first(entries, *refs), [shape, (9, 8, 128), (9, 8, 128)])(
        sums, value, hist_val
    )
    faces = neighbours(GX, *packed)
    edge = (edge_rows(False)[1], 128)
    packed = call(lambda *refs: pack_second(False, *refs), [edge, edge], [(10 * FIELD * 8, 128)])(field, *faces)
    edges = neighbours(GY, *packed)
    value_next, resid, payload = call(second_map, [shape, shape, fan], [frames, *work])(
        field, *faces, *edges, static, hist_res, newest
    )
    (out,) = call(lambda *refs: mix_second(entries, *refs), [shape])(
        exchange(payload), sums, value_next, hist_val, value, value_prev
    )
    return (out, resid)


def build(torus):
    in_specs = (
        P(None, GX, GY, None),
        P(None, GX, GY, None),
        P(GX, GY, None),
        P(None, GX, GY, None),
        P(None, GX, GY, None),
        P(None, None, GX, GY, None),
        P(None, None, GX, GY, None),
    )
    out_specs = (P(None, GX, GY, None), P(None, GX, GY, None))
    return jax.shard_map(local, mesh=torus, in_specs=in_specs, out_specs=out_specs, check_vma=False)


def solution(mesh):
    return build(Mesh(mesh.devices.reshape(2, 16, 2, 2, 8), AXES))
```

```python
import jax
import jax.numpy as jnp
from jax import lax
from jax.experimental import pallas as pl
from jax.experimental.pallas import tpu as pltpu
from jax.sharding import Mesh
from jax.sharding import PartitionSpec as P

M = 5
SWEEPS = 3
AXES = ("gx_0", "gx_1", "gx_2", "gy_0", "gy_1")
GX = ("gx_0", "gx_1", "gx_2")
GY = ("gy_0", "gy_1")
CHAIN = ("gx_1", "gx_2")
PLANE = ("gx_0", "gy_0", "gy_1")

REG = 0.05
FLOOR = 0.001
PAIRS = [(i, j) for i in range(M) for j in range(i, M)]
RHS = len(PAIRS)
PREV = RHS + M
NORM = PREV + M

ROWS = 16
OWN = 3
FIELD = 3
STATIC = 4


def edge_rows(with_static):
    if with_static:
        return [(1, 3, 24, 0, False), (1, 4, 24, 24, True), (2, 8, 16, 48, True), (2, 6, 18, 64, False), (3, 9, 12, 88, False)], 104
    return [(1, 3, 24, 0, False), (2, 6, 18, 24, False), (3, 9, 12, 48, False)], 64


def call(kernel, outs, scratch=(), flops=20000, **more):
    return pl.pallas_call(
        kernel,
        out_shape=[jax.ShapeDtypeStruct(s, jnp.float32) for s in outs],
        scratch_shapes=[pltpu.VMEM(s, jnp.float32) if isinstance(s, tuple) else s for s in scratch],
        compiler_params=pltpu.CompilerParams(vmem_limit_bytes=8 * 1024 * 1024),
        cost_estimate=pl.CostEstimate(flops=flops, bytes_accessed=100000, transcendentals=0),
        **more,
    )


def odd_place(axes):
    return lax.rem(lax.axis_index(axes[-1]), 2) == 1


def pack_first(vel, forcing, visc, even_pair, odd_pair, vel_near, forcing_near, visc_near, sem):
    cx = vel.shape[1]
    odd = odd_place(GX)
    copies = []
    for out, low in ((even_pair, odd), (odd_pair, jnp.logical_not(odd))):
        three = pl.ds(jnp.where(low, 0, cx - 3), 3)
        two = pl.ds(jnp.where(low, 0, cx - 2), 2)
        pieces = [(vel.at[c, three], out.at[pl.ds(3 * c, 3)]) for c in range(3)]
        pieces += [(forcing.at[c, two], out.at[pl.ds(9 + 2 * c, 2)]) for c in range(3)]
        pieces += [(visc.at[two], out.at[pl.ds(15, 2)])]
        for src, dst in pieces:
            copies.append(pltpu.make_async_copy(src, dst, sem.at[len(copies)]))
            copies[-1].start()
    for src, dst in ((vel, vel_near), (forcing, forcing_near), (visc, visc_near)):
        copies.append(pltpu.make_async_copy(src, dst, sem.at[len(copies)]))
        copies[-1].start()
    for copy in copies:
        copy.wait()


def arrived(axes, even_pair, odd_pair):
    odd = odd_place(axes)
    if even_pair.shape != odd_pair.shape:
        even_pair = even_pair.at[jnp.where(odd, 0, 1)]
    before = lambda i: jnp.where(odd, even_pair[i], odd_pair[i])
    after = lambda i: jnp.where(odd, odd_pair[i], even_pair[i])
    return before, after


def field_tile(vel, left, right, tile):
    plane, c = divmod(tile, FIELD)
    cx = vel.shape[1]
    if plane < 3:
        return left(3 * c + plane)
    if plane < 3 + cx:
        return vel[c, plane - 3]
    return right(3 * c + plane - 3 - cx)


def static_tile(forcing, visc, left, right, tile):
    plane, c = divmod(tile, STATIC)
    cx = visc.shape[0]
    if plane < 2:
        return left(9 + 2 * c + plane)
    if plane < 2 + cx:
        return forcing[c, plane - 2] if c < 3 else visc[plane - 2]
    return right(9 + 2 * c + plane - 2 - cx)


def pack_second(with_static, *refs):
    if with_static:
        vel, forcing, visc, near, far, even_pair, odd_pair, tiles, fixed = refs
    else:
        vel, near, far, even_pair, odd_pair, tiles = refs
        fixed = None
    left, right = arrived(GX, near, far)
    if with_static:
        for t in range(8 * STATIC):
            fixed[t * 8 : t * 8 + 8] = static_tile(forcing, visc, left, right, t)
    for t in range(10 * FIELD):
        tiles[t * 8 : t * 8 + 8] = field_tile(vel, left, right, t)
    odd = odd_place(GY)
    pieces, _ = edge_rows(with_static)
    for dist, first, count, row, static in pieces:
        src = fixed if static else tiles
        up = src[pl.ds(first * 8 + 8 - dist, count, stride=8), :]
        down = src[pl.ds(first * 8 + dist - 1, count, stride=8), :]
        even_pair[row : row + count] = jnp.where(odd, down, up)
        odd_pair[row : row + count] = jnp.where(odd, up, down)


def fill_frames(with_static, even_pair, odd_pair, frames, fixed):
    pieces, _ = edge_rows(with_static)
    south, north = arrived(GY, even_pair, odd_pair)
    for dist, first, count, row, static in pieces:
        dst = fixed if static else frames
        dst[pl.ds(first * ROWS + OWN - dist, count, stride=ROWS), :] = south(pl.ds(row, count))
        dst[pl.ds(first * ROWS + OWN + 7 + dist, count, stride=ROWS), :] = north(pl.ds(row, count))


def sweeps(frames, fixed, coef, one, two):
    lane = lax.broadcasted_iota(jnp.int32, (ROWS, 128), 1)
    field = lambda p, c: frames[(p * FIELD + c) * ROWS : (p * FIELD + c + 1) * ROWS]
    still = lambda s, c: fixed[(s * STATIC + c) * ROWS : (s * STATIC + c + 1) * ROWS]
    for s in range(8):
        a = [field(s + 1, c) for c in range(3)]
        visc = still(s, 3)
        inv = 1.0 / (1.0 + 6.0 * visc + jnp.abs(a[0]) + jnp.abs(a[1]) + jnp.abs(a[2]))
        for k in range(3):
            low = (visc + jnp.maximum(a[k], 0.0)) * inv
            high = (visc - jnp.minimum(a[k], 0.0)) * inv
            if k == 2:
                low = jnp.where(lane > 0, low, 0.0)
                high = jnp.where(lane < 127, high, 0.0)
            coef[s, 2 * k] = low
            coef[s, 2 * k + 1] = high
            coef[s, 6 + k] = (still(s, k) + a[k]) * inv

    def relax(src, s, c):
        mid = src(0)
        total = coef[s, 6 + c] + coef[s, 0] * src(-1) + coef[s, 1] * src(1)
        total = total + coef[s, 2] * pltpu.roll(mid, 1, 0) + coef[s, 3] * pltpu.roll(mid, ROWS - 1, 0)
        return total + coef[s, 4] * pltpu.roll(mid, 1, 1) + coef[s, 5] * pltpu.roll(mid, 127, 1)

    for s in range(8):
        for c in range(3):
            one[s, c] = relax(lambda d: field(s + 1 + d, c), s, c)
    for s in range(1, 7):
        for c in range(3):
            two[s, c] = relax(lambda d: one[s + d, c], s, c)
    out = {}
    for s in range(2, 6):
        for c in range(3):
            out[c, s - 2] = relax(lambda d: two[s + d, c], s, c)[OWN : OWN + 8]
    return out


def lanes(row, shape=(1, 128)):
    return lax.broadcasted_iota(jnp.int32, shape, 1)


def spread(row, parts):
    lane = lanes(row)
    for k, part in parts.items():
        whole = jnp.sum(jnp.sum(part, axis=0, keepdims=True), axis=1, keepdims=True)
        row = jnp.where(lane == k, whole, row)
    return row


def gram_part(hist, prev, out):
    tiles = [(c, p) for c in range(3) for p in range(hist.shape[2])]
    parts = {}
    for k, (i, j) in enumerate(PAIRS):
        parts[k] = sum(hist[i, c, p] * hist[j, c, p] for c, p in tiles)
    for i in range(M):
        parts[PREV + i] = sum(hist[i, c, p] * prev[c, p] for c, p in tiles)
    out[...] = spread(jnp.zeros((1, 128), jnp.float32), parts)


def first_map(vel, forcing, visc, near, far, even_pair, odd_pair, hist, prev, gram, value, newest, fixed, payload, frames, coef, one, two):
    frames[...] = jnp.zeros_like(frames)
    fixed[...] = jnp.zeros_like(fixed)
    left, right = arrived(GX, near, far)
    for t in range(8 * STATIC):
        fixed[t * ROWS + OWN : t * ROWS + OWN + 8] = static_tile(forcing, visc, left, right, t)
    for t in range(10 * FIELD):
        frames[t * ROWS + OWN : t * ROWS + OWN + 8] = field_tile(vel, left, right, t)
    fill_frames(True, even_pair, odd_pair, frames, fixed)
    result = sweeps(frames, fixed, coef, one, two)
    resid = {}
    fresh = {}
    for (c, p), tile in result.items():
        value[c, p] = tile
        resid[c, p] = tile - vel[c, p]
        fresh[c, p] = resid[c, p] - prev[c, p]
        newest[c, p] = fresh[c, p]
    parts = {RHS + i: sum(hist[i, c, p] * r for (c, p), r in resid.items()) for i in range(M)}
    parts[NORM] = sum(f * f for f in fresh.values())
    row = spread(gram[...], parts)
    for k in range(payload.shape[0]):
        payload[k] = row


def second_map(vel, near, far, even_pair, odd_pair, fixed, hist, newest, value, resid, payload, frames, coef, one, two):
    frames[...] = jnp.zeros_like(frames)
    left, right = arrived(GX, near, far)
    for t in range(10 * FIELD):
        frames[t * ROWS + OWN : t * ROWS + OWN + 8] = field_tile(vel, left, right, t)
    fill_frames(False, even_pair, odd_pair, frames, None)
    result = sweeps(frames, fixed, coef, one, two)
    for (c, p), tile in result.items():
        value[c, p] = tile
        result[c, p] = tile - vel[c, p]
        resid[c, p] = result[c, p]
    parts = {i: sum(hist[i + 1, c, p] * r for (c, p), r in result.items()) for i in range(M - 1)}
    parts[M - 1] = sum(newest[c, p] * r for (c, p), r in result.items())
    row = spread(jnp.zeros((1, 128), jnp.float32), parts)
    for k in range(payload.shape[0]):
        payload[k] = row


def entry(row, k):
    return jnp.sum(jnp.where(lanes(row) == k, row, 0.0), axis=1, keepdims=True)


def solve(gram, rhs, entries):
    shift = (REG / M) * sum(gram[i, i] for i in range(M)) + FLOOR * entries
    a = {(i, j): gram[min(i, j), max(i, j)] for i in range(M) for j in range(M)}
    for i in range(M):
        a[i, i] = a[i, i] + shift
    r = list(rhs)
    inv = []
    for k in range(M):
        inv.append(1.0 / a[k, k])
        for i in range(k + 1, M):
            f = a[k, i] * inv[k]
            for j in range(i, M):
                a[i, j] = a[i, j] - f * a[k, j]
            r[i] = r[i] - f * r[k]
    out = [None] * M
    for i in reversed(range(M)):
        acc = r[i]
        for j in range(i + 1, M):
            acc = acc - a[i, j] * out[j]
        out[i] = acc * inv[i]
    return out


def gathered(rows):
    total = rows[0]
    for k in range(1, rows.shape[0]):
        total = total + rows[k]
    return total


def mix_first(entries, rows, value, hist, field, even_pair, odd_pair):
    row = gathered(rows)
    s = [entry(row, k) for k in range(PREV)]
    gram = {pair: s[k] for k, pair in enumerate(PAIRS)}
    gamma = [jnp.broadcast_to(g, (8, 128)) for g in solve(gram, s[RHS:PREV], entries)]
    cx = value.shape[1]
    odd = odd_place(GX)
    for c in range(3):
        mixed = []
        for p in range(cx):
            tile = value[c, p]
            for j in range(M):
                tile = tile - gamma[j] * hist[j, c, p]
            field[c, p] = tile
            mixed.append(tile)
        for d in range(3):
            even_pair[3 * c + d] = jnp.where(odd, mixed[d], mixed[cx - 3 + d])
            odd_pair[3 * c + d] = jnp.where(odd, mixed[cx - 3 + d], mixed[d])


def mix_second(entries, rows, first_rows, value, hist, first_value, prev, field):
    row = gathered(first_rows)
    s = [entry(row, k) for k in range(NORM + 1)]
    gram = {}
    for k, (i, j) in enumerate(PAIRS):
        if i > 0:
            gram[i - 1, j - 1] = s[k]
    for i in range(M - 1):
        gram[i, M - 1] = s[RHS + 1 + i] - s[PREV + 1 + i]
    gram[M - 1, M - 1] = s[NORM]
    row = gathered(rows)
    gamma = solve(gram, [entry(row, k) for k in range(M)], entries)
    gamma = [jnp.broadcast_to(g, (8, 128)) for g in gamma]
    for c in range(3):
        for p in range(value.shape[1]):
            tile = value[c, p]
            for j in range(M - 1):
                tile = tile - gamma[j] * hist[j + 1, c, p]
            field[c, p] = tile - gamma[M - 1] * (first_value[c, p] - prev[c, p])


def swap(cells, axes, start):
    pairs = [(i, i + 1) for i in range(start, lax.axis_size(axes) - 1, 2)]
    return lax.ppermute(cells, axes, pairs + [(j, i) for i, j in pairs])


def faces_of(even_pair, odd_pair):
    odd_pair = swap(odd_pair, GX, 1)
    return lax.all_gather(even_pair, GX[2]), odd_pair


def edges_of(even_pair, odd_pair):
    return swap(even_pair, GY, 0), swap(odd_pair, GY, 1)


def exchange(payload):
    row = jnp.sum(lax.all_to_all(payload, CHAIN, 0, 0), axis=(0, 1))
    rows = jnp.broadcast_to(row[None, None, :], (lax.axis_size(PLANE), 1, 128))
    return lax.all_to_all(rows, PLANE, 0, 0)


def local(velocity, forcing, viscosity, residual_prev, value_prev, hist_res, hist_val):
    shape = velocity.shape
    entries = 1.0 * velocity.size * lax.axis_size(GX) * lax.axis_size(GY)
    fan = (lax.axis_size(CHAIN), 1, 128)
    work = ((8, 9, ROWS, 128), (8, 3, ROWS, 128), (8, 3, ROWS, 128))
    frames = (10 * FIELD * ROWS, 128)
    fixed = (8 * STATIC * ROWS, 128)

    hbm = [pl.BlockSpec(memory_space=pltpu.HBM)] * 3
    far_away = [pltpu.with_memory_space_constraint(x, pltpu.HBM) for x in (velocity, forcing, viscosity)]
    *packed, velocity, forcing, viscosity = call(
        pack_first, [(17, 8, 128)] * 2 + [shape, shape, shape[1:]], [pltpu.SemaphoreType.DMA((17,))], in_specs=hbm
    )(*far_away)
    faces = faces_of(*packed)
    (gram,) = call(gram_part, [(1, 128)], flops=4000000)(hist_res, residual_prev)
    edge = (edge_rows(True)[1], 128)
    packed = call(
        lambda *refs: pack_second(True, *refs), [edge, edge], [(10 * FIELD * 8, 128), (8 * STATIC * 8, 128)]
    )(velocity, forcing, viscosity, *faces)
    edges = edges_of(*packed)
    value, newest, static, payload = call(first_map, [shape, shape, fixed, fan], [frames, *work])(
        velocity, forcing, viscosity, *faces, *edges, hist_res, residual_prev, gram
    )
    sums = exchange(payload)
    field, *packed = call(lambda *refs: mix_first(entries, *refs), [shape, (9, 8, 128), (9, 8, 128)])(
        sums, value, hist_val
    )
    faces = faces_of(*packed)
    edge = (edge_rows(False)[1], 128)
    packed = call(lambda *refs: pack_second(False, *refs), [edge, edge], [(10 * FIELD * 8, 128)])(field, *faces)
    edges = edges_of(*packed)
    value_next, resid, payload = call(second_map, [shape, shape, fan], [frames, *work])(
        field, *faces, *edges, static, hist_res, newest
    )
    (out,) = call(lambda *refs: mix_second(entries, *refs), [shape])(
        exchange(payload), sums, value_next, hist_val, value, value_prev
    )
    return (out, resid)


def build(torus):
    in_specs = (
        P(None, GX, GY, None),
        P(None, GX, GY, None),
        P(GX, GY, None),
        P(None, GX, GY, None),
        P(None, GX, GY, None),
        P(None, None, GX, GY, None),
        P(None, None, GX, GY, None),
    )
    out_specs = (P(None, GX, GY, None), P(None, GX, GY, None))
    return jax.shard_map(local, mesh=torus, in_specs=in_specs, out_specs=out_specs, check_vma=False)


def solution(mesh):
    return build(Mesh(mesh.devices.reshape(2, 16, 2, 2, 8), AXES))
```

```python
import jax
import jax.numpy as jnp
from jax import lax
from jax.experimental import pallas as pl
from jax.experimental.pallas import tpu as pltpu
from jax.sharding import Mesh
from jax.sharding import PartitionSpec as P

M = 5
AXES = ("gx_0", "gx_1", "gx_2", "gy_0", "gy_1")
GX = ("gx_0", "gx_1", "gx_2")
GY = ("gy_0", "gy_1")
CHAIN = ("gx_1", "gx_2")
PLANE = ("gx_0", "gy_0", "gy_1")

REG = 0.05
FLOOR = 0.001
PAIRS = [(i, j) for i in range(M) for j in range(i, M)]
RHS = len(PAIRS)
PREV = RHS + M
NORM = PREV + M

ROWS = 16
OWN = 3
FIELD = 3
STATIC = 4


GROUPS = 1 + M
GROUP_ROWS = 56


def edge_rows(with_static):
    if with_static:
        return [(1, 3, 24, 0, False), (1, 4, 24, 24, True), (2, 8, 16, 48, True), (2, 6, 18, 64, False), (3, 9, 12, 88, False)], 104
    return [(1, 3, 24, 0, False), (2, 6, 18, 24, False), (3, 9, 12, 42, False)], GROUP_ROWS


def call(kernel, outs, scratch=(), flops=20000, **more):
    return pl.pallas_call(
        kernel,
        out_shape=[jax.ShapeDtypeStruct(s, jnp.float32) for s in outs],
        scratch_shapes=[pltpu.VMEM(s, jnp.float32) if isinstance(s, tuple) else s for s in scratch],
        compiler_params=pltpu.CompilerParams(vmem_limit_bytes=8 * 1024 * 1024),
        cost_estimate=pl.CostEstimate(flops=flops, bytes_accessed=100000, transcendentals=0),
        **more,
    )


def odd_place(axes):
    return lax.rem(lax.axis_index(axes[-1]), 2) == 1


def pack_first(vel, forcing, visc, even_pair, odd_pair, vel_near, forcing_near, visc_near, sem):
    cx = vel.shape[1]
    odd = odd_place(GX)
    copies = []
    for out, low in ((even_pair, odd), (odd_pair, jnp.logical_not(odd))):
        three = pl.ds(jnp.where(low, 0, cx - 3), 3)
        two = pl.ds(jnp.where(low, 0, cx - 2), 2)
        pieces = [(vel.at[c, three], out.at[pl.ds(3 * c, 3)]) for c in range(3)]
        pieces += [(forcing.at[c, two], out.at[pl.ds(9 + 2 * c, 2)]) for c in range(3)]
        pieces += [(visc.at[two], out.at[pl.ds(15, 2)])]
        for src, dst in pieces:
            copies.append(pltpu.make_async_copy(src, dst, sem.at[len(copies)]))
            copies[-1].start()
    for src, dst in ((vel, vel_near), (forcing, forcing_near), (visc, visc_near)):
        copies.append(pltpu.make_async_copy(src, dst, sem.at[len(copies)]))
        copies[-1].start()
    for copy in copies:
        copy.wait()


def arrived(axes, even_pair, odd_pair):
    odd = odd_place(axes)
    if even_pair.shape != odd_pair.shape:
        even_pair = even_pair.at[jnp.where(odd, 0, 1)]
    before = lambda i: jnp.where(odd, even_pair[i], odd_pair[i])
    after = lambda i: jnp.where(odd, odd_pair[i], even_pair[i])
    return before, after


def field_tile(vel, left, right, tile):
    plane, c = divmod(tile, FIELD)
    cx = vel.shape[1]
    if plane < 3:
        return left(3 * c + plane)
    if plane < 3 + cx:
        return vel[c, plane - 3]
    return right(3 * c + plane - 3 - cx)


def static_tile(forcing, visc, left, right, tile):
    plane, c = divmod(tile, STATIC)
    cx = visc.shape[0]
    if plane < 2:
        return left(9 + 2 * c + plane)
    if plane < 2 + cx:
        return forcing[c, plane - 2] if c < 3 else visc[plane - 2]
    return right(9 + 2 * c + plane - 2 - cx)


def pack_edges(tiles, fixed, even_pair, odd_pair, base, with_static):
    odd = odd_place(GY)
    pieces, _ = edge_rows(with_static)
    for dist, first, count, row, static in pieces:
        src = fixed if static else tiles
        up = src[pl.ds(first * 8 + 8 - dist, count, stride=8), :]
        down = src[pl.ds(first * 8 + dist - 1, count, stride=8), :]
        even_pair[base + row : base + row + count] = jnp.where(odd, down, up)
        odd_pair[base + row : base + row + count] = jnp.where(odd, up, down)


def pack_second(vel, forcing, visc, near, far, even_pair, odd_pair, tiles, fixed):
    left, right = arrived(GX, near, far)
    for t in range(8 * STATIC):
        fixed[t * 8 : t * 8 + 8] = static_tile(forcing, visc, left, right, t)
    for t in range(10 * FIELD):
        tiles[t * 8 : t * 8 + 8] = field_tile(vel, left, right, t)
    pack_edges(tiles, fixed, even_pair, odd_pair, 0, True)


def pack_mixed_first(value, hist, even_pair, odd_pair):
    cx = value.shape[1]
    odd = odd_place(GX)
    for out, low in ((even_pair, odd), (odd_pair, jnp.logical_not(odd))):
        first = jnp.where(low, 0, cx - 3)
        for g in range(GROUPS):
            src = value if g == 0 else hist.at[g - 1]
            for c in range(3):
                for d in range(3):
                    out[9 * g + 3 * c + d] = src[c, first + d]


def pack_mixed_second(value, hist, near, far, even_pair, odd_pair, tiles):
    left, right = arrived(GX, near, far)
    for g in range(GROUPS):
        src = value if g == 0 else hist.at[g - 1]
        block = tiles.at[g]
        for t in range(10 * FIELD):
            block[t * 8 : t * 8 + 8] = field_tile(src, lambda i: left(9 * g + i), lambda i: right(9 * g + i), t)
        pack_edges(block, None, even_pair, odd_pair, g * GROUP_ROWS, False)


def fill_frames(with_static, south, north, frames, fixed):
    pieces, _ = edge_rows(with_static)
    for dist, first, count, row, static in pieces:
        dst = fixed if static else frames
        dst[pl.ds(first * ROWS + OWN - dist, count, stride=ROWS), :] = south(row, count)
        dst[pl.ds(first * ROWS + OWN + 7 + dist, count, stride=ROWS), :] = north(row, count)


def sweeps(frames, fixed, coef, one, two):
    lane = lax.broadcasted_iota(jnp.int32, (ROWS, 128), 1)
    field = lambda p, c: frames[(p * FIELD + c) * ROWS : (p * FIELD + c + 1) * ROWS]
    still = lambda s, c: fixed[(s * STATIC + c) * ROWS : (s * STATIC + c + 1) * ROWS]
    for s in range(8):
        a = [field(s + 1, c) for c in range(3)]
        visc = still(s, 3)
        inv = 1.0 / (1.0 + 6.0 * visc + jnp.abs(a[0]) + jnp.abs(a[1]) + jnp.abs(a[2]))
        for k in range(3):
            low = (visc + jnp.maximum(a[k], 0.0)) * inv
            high = (visc - jnp.minimum(a[k], 0.0)) * inv
            if k == 2:
                low = jnp.where(lane > 0, low, 0.0)
                high = jnp.where(lane < 127, high, 0.0)
            coef[s, 2 * k] = low
            coef[s, 2 * k + 1] = high
            coef[s, 6 + k] = (still(s, k) + a[k]) * inv

    def relax(src, s, c):
        mid = src(0)
        total = coef[s, 6 + c] + coef[s, 0] * src(-1) + coef[s, 1] * src(1)
        total = total + coef[s, 2] * pltpu.roll(mid, 1, 0) + coef[s, 3] * pltpu.roll(mid, ROWS - 1, 0)
        return total + coef[s, 4] * pltpu.roll(mid, 1, 1) + coef[s, 5] * pltpu.roll(mid, 127, 1)

    for s in range(8):
        for c in range(3):
            one[s, c] = relax(lambda d: field(s + 1 + d, c), s, c)
    for s in range(1, 7):
        for c in range(3):
            two[s, c] = relax(lambda d: one[s + d, c], s, c)
    out = {}
    for s in range(2, 6):
        for c in range(3):
            out[c, s - 2] = relax(lambda d: two[s + d, c], s, c)[OWN : OWN + 8]
    return out


def lanes(shape=(1, 128)):
    return lax.broadcasted_iota(jnp.int32, shape, 1)


def spread(row, parts):
    lane = lanes()
    for k, part in parts.items():
        whole = jnp.sum(jnp.sum(part, axis=0, keepdims=True), axis=1, keepdims=True)
        row = jnp.where(lane == k, whole, row)
    return row


def gram_part(hist, prev, out):
    tiles = [(c, p) for c in range(3) for p in range(hist.shape[2])]
    parts = {}
    for k, (i, j) in enumerate(PAIRS):
        parts[k] = sum(hist[i, c, p] * hist[j, c, p] for c, p in tiles)
    for i in range(M):
        parts[PREV + i] = sum(hist[i, c, p] * prev[c, p] for c, p in tiles)
    out[...] = spread(jnp.zeros((1, 128), jnp.float32), parts)


def first_map(vel, forcing, visc, near, far, even_pair, odd_pair, hist, prev, gram, value, newest, fixed, payload, frames, coef, one, two):
    frames[...] = jnp.zeros_like(frames)
    fixed[...] = jnp.zeros_like(fixed)
    left, right = arrived(GX, near, far)
    for t in range(8 * STATIC):
        fixed[t * ROWS + OWN : t * ROWS + OWN + 8] = static_tile(forcing, visc, left, right, t)
    for t in range(10 * FIELD):
        frames[t * ROWS + OWN : t * ROWS + OWN + 8] = field_tile(vel, left, right, t)
    south, north = arrived(GY, even_pair, odd_pair)
    fill_frames(True, lambda r, n: south(pl.ds(r, n)), lambda r, n: north(pl.ds(r, n)), frames, fixed)
    result = sweeps(frames, fixed, coef, one, two)
    resid = {}
    fresh = {}
    for (c, p), tile in result.items():
        value[c, p] = tile
        resid[c, p] = tile - vel[c, p]
        fresh[c, p] = resid[c, p] - prev[c, p]
        newest[c, p] = fresh[c, p]
    parts = {RHS + i: sum(hist[i, c, p] * r for (c, p), r in resid.items()) for i in range(M)}
    parts[NORM] = sum(f * f for f in fresh.values())
    row = spread(gram[...], parts)
    for k in range(payload.shape[0]):
        payload[k] = row


def entry(row, k):
    return jnp.sum(jnp.where(lanes() == k, row, 0.0), axis=1, keepdims=True)


def solve(gram, rhs, entries):
    shift = (REG / M) * sum(gram[i, i] for i in range(M)) + FLOOR * entries
    a = {(i, j): gram[min(i, j), max(i, j)] for i in range(M) for j in range(M)}
    for i in range(M):
        a[i, i] = a[i, i] + shift
    r = list(rhs)
    inv = []
    for k in range(M):
        inv.append(1.0 / a[k, k])
        for i in range(k + 1, M):
            f = a[k, i] * inv[k]
            for j in range(i, M):
                a[i, j] = a[i, j] - f * a[k, j]
            r[i] = r[i] - f * r[k]
    out = [None] * M
    for i in reversed(range(M)):
        acc = r[i]
        for j in range(i + 1, M):
            acc = acc - a[i, j] * out[j]
        out[i] = acc * inv[i]
    return out


def gathered(rows):
    total = rows[0]
    for k in range(1, rows.shape[0]):
        total = total + rows[k]
    return total


def second_map(entries, rows, value, hist_val, near, far, even_pair, odd_pair, fixed, hist, newest, value_next, resid, payload, frames, edges, coef, one, two):
    row = gathered(rows)
    s = [entry(row, k) for k in range(PREV)]
    gram = {pair: s[k] for k, pair in enumerate(PAIRS)}
    gamma = [jnp.broadcast_to(g, (8, 128)) for g in solve(gram, s[RHS:PREV], entries)]

    def mixed(part):
        total = part(0)
        for j in range(M):
            total = total - gamma[j] * part(j + 1)
        return total

    frames[...] = jnp.zeros_like(frames)
    left, right = arrived(GX, near, far)
    field = {}
    for t in range(10 * FIELD):
        plane, c = divmod(t, FIELD)
        tile = mixed(
            lambda g: field_tile(value if g == 0 else hist_val.at[g - 1], lambda i: left(9 * g + i), lambda i: right(9 * g + i), t)
        )
        frames[t * ROWS + OWN : t * ROWS + OWN + 8] = tile
        if 3 <= plane < 7:
            field[c, plane - 3] = tile
    south, north = arrived(GY, even_pair, odd_pair)
    for side, reader in enumerate((south, north)):
        for r in range(0, GROUP_ROWS, 8):
            edges[side, r : r + 8] = mixed(lambda g: reader(pl.ds(g * GROUP_ROWS + r, 8)))
    fill_frames(False, lambda r, n: edges[0, r : r + n], lambda r, n: edges[1, r : r + n], frames, None)
    result = sweeps(frames, fixed, coef, one, two)
    for (c, p), tile in result.items():
        value_next[c, p] = tile
        result[c, p] = tile - field[c, p]
        resid[c, p] = result[c, p]
    parts = {i: sum(hist[i + 1, c, p] * r for (c, p), r in result.items()) for i in range(M - 1)}
    parts[M - 1] = sum(newest[c, p] * r for (c, p), r in result.items())
    row = spread(jnp.zeros((1, 128), jnp.float32), parts)
    for k in range(payload.shape[0]):
        payload[k] = row


def mix_second(entries, rows, first_rows, value, hist, first_value, prev, field):
    row = gathered(first_rows)
    s = [entry(row, k) for k in range(NORM + 1)]
    gram = {}
    for k, (i, j) in enumerate(PAIRS):
        if i > 0:
            gram[i - 1, j - 1] = s[k]
    for i in range(M - 1):
        gram[i, M - 1] = s[RHS + 1 + i] - s[PREV + 1 + i]
    gram[M - 1, M - 1] = s[NORM]
    row = gathered(rows)
    gamma = solve(gram, [entry(row, k) for k in range(M)], entries)
    gamma = [jnp.broadcast_to(g, (8, 128)) for g in gamma]
    for c in range(3):
        for p in range(value.shape[1]):
            tile = value[c, p]
            for j in range(M - 1):
                tile = tile - gamma[j] * hist[j + 1, c, p]
            field[c, p] = tile - gamma[M - 1] * (first_value[c, p] - prev[c, p])


def swap(cells, axes, start):
    pairs = [(i, i + 1) for i in range(start, lax.axis_size(axes) - 1, 2)]
    return lax.ppermute(cells, axes, pairs + [(j, i) for i, j in pairs])


def faces_of(even_pair, odd_pair):
    odd_pair = swap(odd_pair, GX, 1)
    return lax.all_gather(even_pair, GX[2]), odd_pair


def edges_of(even_pair, odd_pair):
    return swap(even_pair, GY, 0), swap(odd_pair, GY, 1)


def exchange(payload):
    rows = lax.all_to_all(payload, CHAIN, 0, 0)
    row = jnp.sum(rows, axis=(0, 1))
    rows = jnp.broadcast_to(row[None, None, :], (lax.axis_size(PLANE), 1, 128))
    return lax.all_to_all(rows, PLANE, 0, 0)


def local(velocity, forcing, viscosity, residual_prev, value_prev, hist_res, hist_val):
    shape = velocity.shape
    entries = 1.0 * velocity.size * lax.axis_size(GX) * lax.axis_size(GY)
    fan = (lax.axis_size(CHAIN), 1, 128)
    work = ((8, 9, ROWS, 128), (8, 3, ROWS, 128), (8, 3, ROWS, 128))
    frames = (10 * FIELD * ROWS, 128)
    fixed = (8 * STATIC * ROWS, 128)

    hbm = [pl.BlockSpec(memory_space=pltpu.HBM)] * 3
    far_away = [pltpu.with_memory_space_constraint(x, pltpu.HBM) for x in (velocity, forcing, viscosity)]
    *packed, velocity, forcing, viscosity = call(
        pack_first, [(17, 8, 128)] * 2 + [shape, shape, shape[1:]], [pltpu.SemaphoreType.DMA((17,))], in_specs=hbm
    )(*far_away)
    faces = faces_of(*packed)
    (gram,) = call(gram_part, [(1, 128)], flops=4000000)(hist_res, residual_prev)
    edge = (edge_rows(True)[1], 128)
    packed = call(pack_second, [edge, edge], [(10 * FIELD * 8, 128), (8 * STATIC * 8, 128)])(
        velocity, forcing, viscosity, *faces
    )
    edges = edges_of(*packed)
    value, newest, static, payload = call(first_map, [shape, shape, fixed, fan], [frames, *work])(
        velocity, forcing, viscosity, *faces, *edges, hist_res, residual_prev, gram
    )
    sums = exchange(payload)
    packed = call(pack_mixed_first, [(9 * GROUPS, 8, 128)] * 2)(value, hist_val)
    faces = faces_of(*packed)
    edge = (GROUPS * GROUP_ROWS, 128)
    packed = call(pack_mixed_second, [edge, edge], [(GROUPS, 10 * FIELD * 8, 128)])(value, hist_val, *faces)
    edges = edges_of(*packed)
    value_next, resid, payload = call(
        lambda *refs: second_map(entries, *refs), [shape, shape, fan], [frames, (2, GROUP_ROWS, 128), *work]
    )(sums, value, hist_val, *faces, *edges, static, hist_res, newest)
    next_sums = exchange(payload)
    (out,) = call(lambda *refs: mix_second(entries, *refs), [shape])(
        next_sums, sums, value_next, hist_val, value, value_prev
    )
    return (out, resid)


def build(torus):
    in_specs = (
        P(None, GX, GY, None),
        P(None, GX, GY, None),
        P(GX, GY, None),
        P(None, GX, GY, None),
        P(None, GX, GY, None),
        P(None, None, GX, GY, None),
        P(None, None, GX, GY, None),
    )
    out_specs = (P(None, GX, GY, None), P(None, GX, GY, None))
    return jax.shard_map(local, mesh=torus, in_specs=in_specs, out_specs=out_specs, check_vma=False)


def solution(mesh):
    torus = Mesh(mesh.devices.reshape(2, 16, 2, 2, 8), AXES)
    return build(torus)
```

```python
import jax
import jax.numpy as jnp
from jax import lax
from jax.experimental import pallas as pl
from jax.experimental.pallas import tpu as pltpu
from jax.sharding import Mesh
from jax.sharding import PartitionSpec as P

M = 5
AXES = ("gx_0", "gx_1", "gx_2", "gy_0", "gy_1")
GX = ("gx_0", "gx_1", "gx_2")
GY = ("gy_0", "gy_1")
CHAIN = ("gx_1", "gx_2")
PLANE = ("gx_0", "gy_0", "gy_1")

REG = 0.05
FLOOR = 0.001
PAIRS = [(i, j) for i in range(M) for j in range(i, M)]
RHS = len(PAIRS)
PREV = RHS + M
NORM = PREV + M

ROWS = 16
OWN = 3
FIELD = 3
STATIC = 4


GROUPS = 1 + M
GROUP_ROWS = 56


def edge_rows(with_static):
    if with_static:
        return [(1, 3, 24, 0, False), (1, 4, 24, 24, True), (2, 8, 16, 48, True), (2, 6, 18, 64, False), (3, 9, 12, 88, False)], 104
    return [(1, 3, 24, 0, False), (2, 6, 18, 24, False), (3, 9, 12, 42, False)], GROUP_ROWS


def call(kernel, outs, scratch=(), flops=20000, **more):
    return pl.pallas_call(
        kernel,
        out_shape=[jax.ShapeDtypeStruct(s, jnp.float32) for s in outs],
        scratch_shapes=[pltpu.VMEM(s, jnp.float32) if isinstance(s, tuple) else s for s in scratch],
        compiler_params=pltpu.CompilerParams(vmem_limit_bytes=8 * 1024 * 1024),
        cost_estimate=pl.CostEstimate(flops=flops, bytes_accessed=100000, transcendentals=0),
        **more,
    )


def odd_place(axes):
    return lax.rem(lax.axis_index(axes[-1]), 2) == 1


def pack_first(vel, forcing, visc, even_pair, odd_pair, vel_near, forcing_near, visc_near, sem):
    cx = vel.shape[1]
    odd = odd_place(GX)
    copies = []
    for out, low in ((even_pair, odd), (odd_pair, jnp.logical_not(odd))):
        three = pl.ds(jnp.where(low, 0, cx - 3), 3)
        two = pl.ds(jnp.where(low, 0, cx - 2), 2)
        pieces = [(vel.at[c, three], out.at[pl.ds(3 * c, 3)]) for c in range(3)]
        pieces += [(forcing.at[c, two], out.at[pl.ds(9 + 2 * c, 2)]) for c in range(3)]
        pieces += [(visc.at[two], out.at[pl.ds(15, 2)])]
        for src, dst in pieces:
            copies.append(pltpu.make_async_copy(src, dst, sem.at[len(copies)]))
            copies[-1].start()
    for src, dst in ((vel, vel_near), (forcing, forcing_near), (visc, visc_near)):
        copies.append(pltpu.make_async_copy(src, dst, sem.at[len(copies)]))
        copies[-1].start()
    for copy in copies:
        copy.wait()


def arrived(axes, even_pair, odd_pair):
    odd = odd_place(axes)
    if even_pair.shape != odd_pair.shape:
        even_pair = even_pair.at[jnp.where(odd, 0, 1)]
    before = lambda i: jnp.where(odd, even_pair[i], odd_pair[i])
    after = lambda i: jnp.where(odd, odd_pair[i], even_pair[i])
    return before, after


def field_tile(vel, left, right, tile):
    plane, c = divmod(tile, FIELD)
    cx = vel.shape[1]
    if plane < 3:
        return left(3 * c + plane)
    if plane < 3 + cx:
        return vel[c, plane - 3]
    return right(3 * c + plane - 3 - cx)


def static_tile(forcing, visc, left, right, tile):
    plane, c = divmod(tile, STATIC)
    cx = visc.shape[0]
    if plane < 2:
        return left(9 + 2 * c + plane)
    if plane < 2 + cx:
        return forcing[c, plane - 2] if c < 3 else visc[plane - 2]
    return right(9 + 2 * c + plane - 2 - cx)


def pack_edges(tiles, fixed, even_pair, odd_pair, base, with_static):
    odd = odd_place(GY)
    pieces, _ = edge_rows(with_static)
    for dist, first, count, row, static in pieces:
        src = fixed if static else tiles
        up = src[pl.ds(first * 8 + 8 - dist, count, stride=8), :]
        down = src[pl.ds(first * 8 + dist - 1, count, stride=8), :]
        even_pair[base + row : base + row + count] = jnp.where(odd, down, up)
        odd_pair[base + row : base + row + count] = jnp.where(odd, up, down)


def pack_second(vel, forcing, visc, near, far, even_pair, odd_pair, tiles, fixed):
    left, right = arrived(GX, near, far)
    for t in range(8 * STATIC):
        fixed[t * 8 : t * 8 + 8] = static_tile(forcing, visc, left, right, t)
    for t in range(10 * FIELD):
        tiles[t * 8 : t * 8 + 8] = field_tile(vel, left, right, t)
    pack_edges(tiles, fixed, even_pair, odd_pair, 0, True)


def pack_mixed_first(value, hist, even_pair, odd_pair):
    cx = value.shape[1]
    odd = odd_place(GX)
    for out, low in ((even_pair, odd), (odd_pair, jnp.logical_not(odd))):
        first = jnp.where(low, 0, cx - 3)
        for g in range(GROUPS):
            src = value if g == 0 else hist.at[g - 1]
            for c in range(3):
                for d in range(3):
                    out[9 * g + 3 * c + d] = src[c, first + d]


def pack_mixed_second(value, hist, near, far, even_pair, odd_pair, tiles):
    left, right = arrived(GX, near, far)
    for g in range(GROUPS):
        src = value if g == 0 else hist.at[g - 1]
        block = tiles.at[g]
        for t in range(10 * FIELD):
            block[t * 8 : t * 8 + 8] = field_tile(src, lambda i: left(9 * g + i), lambda i: right(9 * g + i), t)
        pack_edges(block, None, even_pair, odd_pair, g * GROUP_ROWS, False)


def fill_frames(with_static, south, north, frames, fixed):
    pieces, _ = edge_rows(with_static)
    for dist, first, count, row, static in pieces:
        dst = fixed if static else frames
        dst[pl.ds(first * ROWS + OWN - dist, count, stride=ROWS), :] = south(row, count)
        dst[pl.ds(first * ROWS + OWN + 7 + dist, count, stride=ROWS), :] = north(row, count)


def sweeps(frames, fixed, coef, one, two):
    lane = lax.broadcasted_iota(jnp.int32, (ROWS, 128), 1)
    field = lambda p, c: frames[(p * FIELD + c) * ROWS : (p * FIELD + c + 1) * ROWS]
    still = lambda s, c: fixed[(s * STATIC + c) * ROWS : (s * STATIC + c + 1) * ROWS]
    for s in range(8):
        a = [field(s + 1, c) for c in range(3)]
        visc = still(s, 3)
        inv = 1.0 / (1.0 + 6.0 * visc + jnp.abs(a[0]) + jnp.abs(a[1]) + jnp.abs(a[2]))
        for k in range(3):
            low = (visc + jnp.maximum(a[k], 0.0)) * inv
            high = (visc - jnp.minimum(a[k], 0.0)) * inv
            if k == 2:
                low = jnp.where(lane > 0, low, 0.0)
                high = jnp.where(lane < 127, high, 0.0)
            coef[s, 2 * k] = low
            coef[s, 2 * k + 1] = high
            coef[s, 6 + k] = (still(s, k) + a[k]) * inv

    def relax(src, s, c):
        mid = src(0)
        total = coef[s, 6 + c] + coef[s, 0] * src(-1) + coef[s, 1] * src(1)
        total = total + coef[s, 2] * pltpu.roll(mid, 1, 0) + coef[s, 3] * pltpu.roll(mid, ROWS - 1, 0)
        return total + coef[s, 4] * pltpu.roll(mid, 1, 1) + coef[s, 5] * pltpu.roll(mid, 127, 1)

    for s in range(8):
        for c in range(3):
            one[s, c] = relax(lambda d: field(s + 1 + d, c), s, c)
    for s in range(1, 7):
        for c in range(3):
            two[s, c] = relax(lambda d: one[s + d, c], s, c)
    out = {}
    for s in range(2, 6):
        for c in range(3):
            out[c, s - 2] = relax(lambda d: two[s + d, c], s, c)[OWN : OWN + 8]
    return out


def lanes(shape=(1, 128)):
    return lax.broadcasted_iota(jnp.int32, shape, 1)


def spread(row, parts):
    lane = lanes()
    for k, part in parts.items():
        whole = jnp.sum(jnp.sum(part, axis=0, keepdims=True), axis=1, keepdims=True)
        row = jnp.where(lane == k, whole, row)
    return row


def gram_part(hist, prev, out):
    tiles = [(c, p) for c in range(3) for p in range(hist.shape[2])]
    parts = {}
    for k, (i, j) in enumerate(PAIRS):
        parts[k] = sum(hist[i, c, p] * hist[j, c, p] for c, p in tiles)
    for i in range(M):
        parts[PREV + i] = sum(hist[i, c, p] * prev[c, p] for c, p in tiles)
    out[...] = spread(jnp.zeros((1, 128), jnp.float32), parts)


def first_map(vel, forcing, visc, near, far, even_pair, odd_pair, hist, prev, gram, value, newest, fixed, payload, frames, coef, one, two):
    frames[...] = jnp.zeros_like(frames)
    fixed[...] = jnp.zeros_like(fixed)
    left, right = arrived(GX, near, far)
    for t in range(8 * STATIC):
        fixed[t * ROWS + OWN : t * ROWS + OWN + 8] = static_tile(forcing, visc, left, right, t)
    for t in range(10 * FIELD):
        frames[t * ROWS + OWN : t * ROWS + OWN + 8] = field_tile(vel, left, right, t)
    south, north = arrived(GY, even_pair, odd_pair)
    fill_frames(True, lambda r, n: south(pl.ds(r, n)), lambda r, n: north(pl.ds(r, n)), frames, fixed)
    result = sweeps(frames, fixed, coef, one, two)
    resid = {}
    fresh = {}
    for (c, p), tile in result.items():
        value[c, p] = tile
        resid[c, p] = tile - vel[c, p]
        fresh[c, p] = resid[c, p] - prev[c, p]
        newest[c, p] = fresh[c, p]
    parts = {RHS + i: sum(hist[i, c, p] * r for (c, p), r in resid.items()) for i in range(M)}
    parts[NORM] = sum(f * f for f in fresh.values())
    row = spread(gram[...], parts)
    for k in range(payload.shape[0]):
        payload[k] = row


def entry(row, k):
    return jnp.sum(jnp.where(lanes() == k, row, 0.0), axis=1, keepdims=True)


def solve(gram, rhs, entries):
    shift = (REG / M) * sum(gram[i, i] for i in range(M)) + FLOOR * entries
    a = {(i, j): gram[min(i, j), max(i, j)] for i in range(M) for j in range(M)}
    for i in range(M):
        a[i, i] = a[i, i] + shift
    r = list(rhs)
    inv = []
    for k in range(M):
        inv.append(1.0 / a[k, k])
        for i in range(k + 1, M):
            f = a[k, i] * inv[k]
            for j in range(i, M):
                a[i, j] = a[i, j] - f * a[k, j]
            r[i] = r[i] - f * r[k]
    out = [None] * M
    for i in reversed(range(M)):
        acc = r[i]
        for j in range(i + 1, M):
            acc = acc - a[i, j] * out[j]
        out[i] = acc * inv[i]
    return out


def gathered(rows):
    total = rows[0]
    for k in range(1, rows.shape[0]):
        total = total + rows[k]
    return total


def second_map(entries, rows, value, hist_val, near, far, even_pair, odd_pair, fixed, hist, newest, value_next, resid, payload, frames, edges, coef, one, two):
    row = gathered(rows)
    s = [entry(row, k) for k in range(PREV)]
    gram = {pair: s[k] for k, pair in enumerate(PAIRS)}
    gamma = [jnp.broadcast_to(g, (8, 128)) for g in solve(gram, s[RHS:PREV], entries)]

    def mixed(part):
        total = part(0)
        for j in range(M):
            total = total - gamma[j] * part(j + 1)
        return total

    frames[...] = jnp.zeros_like(frames)
    left, right = arrived(GX, near, far)
    field = {}
    for t in range(10 * FIELD):
        plane, c = divmod(t, FIELD)
        tile = mixed(
            lambda g: field_tile(value if g == 0 else hist_val.at[g - 1], lambda i: left(9 * g + i), lambda i: right(9 * g + i), t)
        )
        frames[t * ROWS + OWN : t * ROWS + OWN + 8] = tile
        if 3 <= plane < 7:
            field[c, plane - 3] = tile
    south, north = arrived(GY, even_pair, odd_pair)
    for side, reader in enumerate((south, north)):
        for r in range(0, GROUP_ROWS, 8):
            edges[side, r : r + 8] = mixed(lambda g: reader(pl.ds(g * GROUP_ROWS + r, 8)))
    fill_frames(False, lambda r, n: edges[0, r : r + n], lambda r, n: edges[1, r : r + n], frames, None)
    result = sweeps(frames, fixed, coef, one, two)
    for (c, p), tile in result.items():
        value_next[c, p] = tile
        result[c, p] = tile - field[c, p]
        resid[c, p] = result[c, p]
    parts = {i: sum(hist[i + 1, c, p] * r for (c, p), r in result.items()) for i in range(M - 1)}
    parts[M - 1] = sum(newest[c, p] * r for (c, p), r in result.items())
    row = spread(jnp.zeros((1, 128), jnp.float32), parts)
    for k in range(payload.shape[0]):
        payload[k] = row


def mix_second(entries, rows, first_rows, value, hist, first_value, prev, resid, field, resid_out):
    resid_out[...] = resid[...]
    row = gathered(first_rows)
    s = [entry(row, k) for k in range(NORM + 1)]
    gram = {}
    for k, (i, j) in enumerate(PAIRS):
        if i > 0:
            gram[i - 1, j - 1] = s[k]
    for i in range(M - 1):
        gram[i, M - 1] = s[RHS + 1 + i] - s[PREV + 1 + i]
    gram[M - 1, M - 1] = s[NORM]
    row = gathered(rows)
    gamma = solve(gram, [entry(row, k) for k in range(M)], entries)
    gamma = [jnp.broadcast_to(g, (8, 128)) for g in gamma]
    for c in range(3):
        for p in range(value.shape[1]):
            tile = value[c, p]
            for j in range(M - 1):
                tile = tile - gamma[j] * hist[j + 1, c, p]
            field[c, p] = tile - gamma[M - 1] * (first_value[c, p] - prev[c, p])


def swap(cells, axes, start):
    pairs = [(i, i + 1) for i in range(start, lax.axis_size(axes) - 1, 2)]
    return lax.ppermute(cells, axes, pairs + [(j, i) for i, j in pairs])


def faces_of(even_pair, odd_pair):
    odd_pair = swap(odd_pair, GX, 1)
    return lax.all_gather(even_pair, GX[2]), odd_pair


def edges_of(even_pair, odd_pair):
    even_pair = swap(even_pair, GY, 0)
    odd_pair = swap(odd_pair, GY, 1)
    return even_pair, odd_pair


def exchange(payload):
    rows = lax.all_to_all(payload, CHAIN, 0, 0)
    row = jnp.sum(rows, axis=(0, 1))
    rows = jnp.broadcast_to(row[None, None, :], (lax.axis_size(PLANE), 1, 128))
    return lax.all_to_all(rows, PLANE, 0, 0)


def local(velocity, forcing, viscosity, residual_prev, value_prev, hist_res, hist_val):
    shape = velocity.shape
    entries = 1.0 * velocity.size * lax.axis_size(GX) * lax.axis_size(GY)
    fan = (lax.axis_size(CHAIN), 1, 128)
    work = ((8, 9, ROWS, 128), (8, 3, ROWS, 128), (8, 3, ROWS, 128))
    frames = (10 * FIELD * ROWS, 128)
    fixed = (8 * STATIC * ROWS, 128)

    hbm = [pl.BlockSpec(memory_space=pltpu.HBM)] * 3
    far_away = [pltpu.with_memory_space_constraint(x, pltpu.HBM) for x in (velocity, forcing, viscosity)]
    *packed, velocity, forcing, viscosity = call(
        pack_first, [(17, 8, 128)] * 2 + [shape, shape, shape[1:]], [pltpu.SemaphoreType.DMA((17,))], in_specs=hbm
    )(*far_away)
    faces = faces_of(*packed)
    (gram,) = call(gram_part, [(1, 128)], flops=4000000)(hist_res, residual_prev)
    edge = (edge_rows(True)[1], 128)
    packed = call(pack_second, [edge, edge], [(10 * FIELD * 8, 128), (8 * STATIC * 8, 128)])(
        velocity, forcing, viscosity, *faces
    )
    edges = edges_of(*packed)
    value, newest, static, payload = call(first_map, [shape, shape, fixed, fan], [frames, *work])(
        velocity, forcing, viscosity, *faces, *edges, hist_res, residual_prev, gram
    )
    sums = exchange(payload)
    packed = call(pack_mixed_first, [(9 * GROUPS, 8, 128)] * 2)(value, hist_val)
    faces = faces_of(*packed)
    edge = (GROUPS * GROUP_ROWS, 128)
    packed = call(pack_mixed_second, [edge, edge], [(GROUPS, 10 * FIELD * 8, 128)])(value, hist_val, *faces)
    edges = edges_of(*packed)
    value_next, resid, payload = call(
        lambda *refs: second_map(entries, *refs), [shape, shape, fan], [frames, (2, GROUP_ROWS, 128), *work]
    )(sums, value, hist_val, *faces, *edges, static, hist_res, newest)
    next_sums = exchange(payload)
    return call(lambda *refs: mix_second(entries, *refs), [shape, shape])(
        next_sums, sums, value_next, hist_val, value, value_prev, resid
    )


def build(torus):
    in_specs = (
        P(None, GX, GY, None),
        P(None, GX, GY, None),
        P(GX, GY, None),
        P(None, GX, GY, None),
        P(None, GX, GY, None),
        P(None, None, GX, GY, None),
        P(None, None, GX, GY, None),
    )
    out_specs = (P(None, GX, GY, None), P(None, GX, GY, None))
    return jax.shard_map(local, mesh=torus, in_specs=in_specs, out_specs=out_specs, check_vma=False)


def solution(mesh):
    torus = Mesh(mesh.devices.reshape(2, 16, 2, 2, 8), AXES)
    return build(torus)
```

```python
import jax
import jax.numpy as jnp
from jax import lax
from jax.experimental import pallas as pl
from jax.experimental.pallas import tpu as pltpu
from jax.sharding import Mesh
from jax.sharding import PartitionSpec as P

M = 5
AXES = ("gx_0", "gx_1", "gx_2", "gy_0", "gy_1")
GX = ("gx_0", "gx_1", "gx_2")
GY = ("gy_0", "gy_1")
CHAIN = ("gx_1", "gx_2")
PLANE = ("gx_0", "gy_0", "gy_1")

REG = 0.05
FLOOR = 0.001
PAIRS = [(i, j) for i in range(M) for j in range(i, M)]
RHS = len(PAIRS)
PREV = RHS + M
NORM = PREV + M

ROWS = 16
OWN = 3
FIELD = 3
STATIC = 4


GROUPS = 1 + M
GROUP_ROWS = 56


def edge_rows(with_static):
    if with_static:
        return [(1, 3, 24, 0, False), (1, 4, 24, 24, True), (2, 8, 16, 48, True), (2, 6, 18, 64, False), (3, 9, 12, 88, False)], 104
    return [(1, 3, 24, 0, False), (2, 6, 18, 24, False), (3, 9, 12, 42, False)], GROUP_ROWS


def call(kernel, outs, scratch=(), flops=20000, **more):
    return pl.pallas_call(
        kernel,
        out_shape=[jax.ShapeDtypeStruct(s, jnp.float32) for s in outs],
        scratch_shapes=[pltpu.VMEM(s, jnp.float32) if isinstance(s, tuple) else s for s in scratch],
        compiler_params=pltpu.CompilerParams(vmem_limit_bytes=8 * 1024 * 1024),
        cost_estimate=pl.CostEstimate(flops=flops, bytes_accessed=100000, transcendentals=0),
        **more,
    )


def odd_place(axes):
    return lax.rem(lax.axis_index(axes[-1]), 2) == 1


def pack_first(vel, forcing, visc, hist, even_pair, odd_pair, vel_near, forcing_near, visc_near, sem):
    cx = vel.shape[1]
    odd = odd_place(GX)
    copies = []
    for out, low in ((even_pair, odd), (odd_pair, jnp.logical_not(odd))):
        three = pl.ds(jnp.where(low, 0, cx - 3), 3)
        two = pl.ds(jnp.where(low, 0, cx - 2), 2)
        pieces = [(vel.at[c, three], out.at[pl.ds(3 * c, 3)]) for c in range(3)]
        pieces += [(forcing.at[c, two], out.at[pl.ds(9 + 2 * c, 2)]) for c in range(3)]
        pieces += [(visc.at[two], out.at[pl.ds(15, 2)])]
        if out is even_pair:
            pieces += [(hist.at[j, c, three], out.at[pl.ds(17 + 9 * j + 3 * c, 3)]) for j in range(M) for c in range(3)]
        for src, dst in pieces:
            copies.append(pltpu.make_async_copy(src, dst, sem.at[len(copies)]))
            copies[-1].start()
    for src, dst in ((vel, vel_near), (forcing, forcing_near), (visc, visc_near)):
        copies.append(pltpu.make_async_copy(src, dst, sem.at[len(copies)]))
        copies[-1].start()
    for copy in copies:
        copy.wait()


def arrived(axes, even_pair, odd_pair):
    odd = odd_place(axes)
    if even_pair.shape != odd_pair.shape:
        even_pair = even_pair.at[jnp.where(odd, 0, 1)]
    before = lambda i: jnp.where(odd, even_pair[i], odd_pair[i])
    after = lambda i: jnp.where(odd, odd_pair[i], even_pair[i])
    return before, after


def field_tile(vel, left, right, tile):
    plane, c = divmod(tile, FIELD)
    cx = vel.shape[1]
    if plane < 3:
        return left(3 * c + plane)
    if plane < 3 + cx:
        return vel[c, plane - 3]
    return right(3 * c + plane - 3 - cx)


def static_tile(forcing, visc, left, right, tile):
    plane, c = divmod(tile, STATIC)
    cx = visc.shape[0]
    if plane < 2:
        return left(9 + 2 * c + plane)
    if plane < 2 + cx:
        return forcing[c, plane - 2] if c < 3 else visc[plane - 2]
    return right(9 + 2 * c + plane - 2 - cx)


def pack_edges(tiles, fixed, even_pair, odd_pair, base, with_static):
    odd = odd_place(GY)
    pieces, _ = edge_rows(with_static)
    for dist, first, count, row, static in pieces:
        src = fixed if static else tiles
        up = src[pl.ds(first * 8 + 8 - dist, count, stride=8), :]
        down = src[pl.ds(first * 8 + dist - 1, count, stride=8), :]
        even_pair[base + row : base + row + count] = jnp.where(odd, down, up)
        odd_pair[base + row : base + row + count] = jnp.where(odd, up, down)


def pack_second(vel, forcing, visc, near, far, even_pair, odd_pair, tiles, fixed):
    left, right = arrived(GX, near, far)
    for t in range(8 * STATIC):
        fixed[t * 8 : t * 8 + 8] = static_tile(forcing, visc, left, right, t)
    for t in range(10 * FIELD):
        tiles[t * 8 : t * 8 + 8] = field_tile(vel, left, right, t)
    pack_edges(tiles, fixed, even_pair, odd_pair, 0, True)


def pack_faces(field, even_pair, odd_pair):
    cx = field.shape[-3]
    odd = odd_place(GX)
    for out, low in ((even_pair, odd), (odd_pair, jnp.logical_not(odd))):
        if out is not None:
            first = jnp.where(low, 0, cx - 3)
            for g in range(out.shape[0] // 9):
                src = field.at[g] if len(field.shape) == 5 else field
                for c in range(3):
                    for d in range(3):
                        out[9 * g + 3 * c + d] = src[c, first + d]


def mixed_sides(near, near_value, far_value, far_hist):
    odd = odd_place(GX)
    near = near.at[jnp.where(odd, 0, 1)]
    near_value = near_value.at[jnp.where(odd, 0, 1)]
    even_pair = lambda i: near_value[i] if i < 9 else near[17 + i - 9]
    odd_pair = lambda i: far_value[i] if i < 9 else far_hist[i - 9]
    before = lambda i: jnp.where(odd, even_pair(i), odd_pair(i))
    after = lambda i: jnp.where(odd, odd_pair(i), even_pair(i))
    return before, after


def pack_mixed_second(value, hist, near, near_value, far_value, far_hist, even_pair, odd_pair, tiles):
    left, right = mixed_sides(near, near_value, far_value, far_hist)
    for g in range(GROUPS):
        src = value if g == 0 else hist.at[g - 1]
        block = tiles.at[g]
        for t in range(10 * FIELD):
            block[t * 8 : t * 8 + 8] = field_tile(src, lambda i: left(9 * g + i), lambda i: right(9 * g + i), t)
        pack_edges(block, None, even_pair, odd_pair, g * GROUP_ROWS, False)


def fill_frames(with_static, south, north, frames, fixed):
    pieces, _ = edge_rows(with_static)
    for dist, first, count, row, static in pieces:
        dst = fixed if static else frames
        dst[pl.ds(first * ROWS + OWN - dist, count, stride=ROWS), :] = south(row, count)
        dst[pl.ds(first * ROWS + OWN + 7 + dist, count, stride=ROWS), :] = north(row, count)


def sweeps(frames, fixed, coef, one, two):
    lane = lax.broadcasted_iota(jnp.int32, (ROWS, 128), 1)
    field = lambda p, c: frames[(p * FIELD + c) * ROWS : (p * FIELD + c + 1) * ROWS]
    still = lambda s, c: fixed[(s * STATIC + c) * ROWS : (s * STATIC + c + 1) * ROWS]
    for s in range(8):
        a = [field(s + 1, c) for c in range(3)]
        visc = still(s, 3)
        inv = 1.0 / (1.0 + 6.0 * visc + jnp.abs(a[0]) + jnp.abs(a[1]) + jnp.abs(a[2]))
        for k in range(3):
            low = (visc + jnp.maximum(a[k], 0.0)) * inv
            high = (visc - jnp.minimum(a[k], 0.0)) * inv
            if k == 2:
                low = jnp.where(lane > 0, low, 0.0)
                high = jnp.where(lane < 127, high, 0.0)
            coef[s, 2 * k] = low
            coef[s, 2 * k + 1] = high
            coef[s, 6 + k] = (still(s, k) + a[k]) * inv

    def relax(src, s, c):
        mid = src(0)
        total = coef[s, 6 + c] + coef[s, 0] * src(-1) + coef[s, 1] * src(1)
        total = total + coef[s, 2] * pltpu.roll(mid, 1, 0) + coef[s, 3] * pltpu.roll(mid, ROWS - 1, 0)
        return total + coef[s, 4] * pltpu.roll(mid, 1, 1) + coef[s, 5] * pltpu.roll(mid, 127, 1)

    for s in range(8):
        for c in range(3):
            one[s, c] = relax(lambda d: field(s + 1 + d, c), s, c)
    for s in range(1, 7):
        for c in range(3):
            two[s, c] = relax(lambda d: one[s + d, c], s, c)
    out = {}
    for s in range(2, 6):
        for c in range(3):
            out[c, s - 2] = relax(lambda d: two[s + d, c], s, c)[OWN : OWN + 8]
    return out


def lanes(shape=(1, 128)):
    return lax.broadcasted_iota(jnp.int32, shape, 1)


def spread(row, parts):
    lane = lanes()
    for k, part in parts.items():
        whole = jnp.sum(jnp.sum(part, axis=0, keepdims=True), axis=1, keepdims=True)
        row = jnp.where(lane == k, whole, row)
    return row


def gram_part(hist, prev, out):
    tiles = [(c, p) for c in range(3) for p in range(hist.shape[2])]
    parts = {}
    for k, (i, j) in enumerate(PAIRS):
        parts[k] = sum(hist[i, c, p] * hist[j, c, p] for c, p in tiles)
    for i in range(M):
        parts[PREV + i] = sum(hist[i, c, p] * prev[c, p] for c, p in tiles)
    out[...] = spread(jnp.zeros((1, 128), jnp.float32), parts)


def first_map(vel, forcing, visc, near, far, even_pair, odd_pair, hist, prev, gram, value, newest, fixed, payload, frames, coef, one, two):
    frames[...] = jnp.zeros_like(frames)
    fixed[...] = jnp.zeros_like(fixed)
    left, right = arrived(GX, near, far)
    for t in range(8 * STATIC):
        fixed[t * ROWS + OWN : t * ROWS + OWN + 8] = static_tile(forcing, visc, left, right, t)
    for t in range(10 * FIELD):
        frames[t * ROWS + OWN : t * ROWS + OWN + 8] = field_tile(vel, left, right, t)
    south, north = arrived(GY, even_pair, odd_pair)
    fill_frames(True, lambda r, n: south(pl.ds(r, n)), lambda r, n: north(pl.ds(r, n)), frames, fixed)
    result = sweeps(frames, fixed, coef, one, two)
    resid = {}
    fresh = {}
    for (c, p), tile in result.items():
        value[c, p] = tile
        resid[c, p] = tile - vel[c, p]
        fresh[c, p] = resid[c, p] - prev[c, p]
        newest[c, p] = fresh[c, p]
    parts = {RHS + i: sum(hist[i, c, p] * r for (c, p), r in resid.items()) for i in range(M)}
    parts[NORM] = sum(f * f for f in fresh.values())
    row = spread(gram[...], parts)
    for k in range(payload.shape[0]):
        payload[k] = row


def entry(row, k):
    return jnp.sum(jnp.where(lanes() == k, row, 0.0), axis=1, keepdims=True)


def solve(gram, rhs, entries):
    shift = (REG / M) * sum(gram[i, i] for i in range(M)) + FLOOR * entries
    a = {(i, j): gram[min(i, j), max(i, j)] for i in range(M) for j in range(M)}
    for i in range(M):
        a[i, i] = a[i, i] + shift
    r = list(rhs)
    inv = []
    for k in range(M):
        inv.append(1.0 / a[k, k])
        for i in range(k + 1, M):
            f = a[k, i] * inv[k]
            for j in range(i, M):
                a[i, j] = a[i, j] - f * a[k, j]
            r[i] = r[i] - f * r[k]
    out = [None] * M
    for i in reversed(range(M)):
        acc = r[i]
        for j in range(i + 1, M):
            acc = acc - a[i, j] * out[j]
        out[i] = acc * inv[i]
    return out


def gathered(rows):
    total = rows[0]
    for k in range(1, rows.shape[0]):
        total = total + rows[k]
    return total


def second_map(entries, rows, value, hist_val, near, near_value, far_value, far_hist, even_pair, odd_pair, fixed, hist, newest, value_next, resid, payload, frames, edges, coef, one, two):
    row = gathered(rows)
    s = [entry(row, k) for k in range(PREV)]
    gram = {pair: s[k] for k, pair in enumerate(PAIRS)}
    gamma = [jnp.broadcast_to(g, (8, 128)) for g in solve(gram, s[RHS:PREV], entries)]

    def mixed(part):
        total = part(0)
        for j in range(M):
            total = total - gamma[j] * part(j + 1)
        return total

    frames[...] = jnp.zeros_like(frames)
    left, right = mixed_sides(near, near_value, far_value, far_hist)
    field = {}
    for t in range(10 * FIELD):
        plane, c = divmod(t, FIELD)
        tile = mixed(
            lambda g: field_tile(value if g == 0 else hist_val.at[g - 1], lambda i: left(9 * g + i), lambda i: right(9 * g + i), t)
        )
        frames[t * ROWS + OWN : t * ROWS + OWN + 8] = tile
        if 3 <= plane < 7:
            field[c, plane - 3] = tile
    south, north = arrived(GY, even_pair, odd_pair)
    for side, reader in enumerate((south, north)):
        for r in range(0, GROUP_ROWS, 8):
            edges[side, r : r + 8] = mixed(lambda g: reader(pl.ds(g * GROUP_ROWS + r, 8)))
    fill_frames(False, lambda r, n: edges[0, r : r + n], lambda r, n: edges[1, r : r + n], frames, None)
    result = sweeps(frames, fixed, coef, one, two)
    for (c, p), tile in result.items():
        value_next[c, p] = tile
        result[c, p] = tile - field[c, p]
        resid[c, p] = result[c, p]
    parts = {i: sum(hist[i + 1, c, p] * r for (c, p), r in result.items()) for i in range(M - 1)}
    parts[M - 1] = sum(newest[c, p] * r for (c, p), r in result.items())
    row = spread(jnp.zeros((1, 128), jnp.float32), parts)
    for k in range(payload.shape[0]):
        payload[k] = row


def mix_second(entries, rows, first_rows, value, hist, first_value, prev, resid, field, resid_out):
    resid_out[...] = resid[...]
    row = gathered(first_rows)
    s = [entry(row, k) for k in range(NORM + 1)]
    gram = {}
    for k, (i, j) in enumerate(PAIRS):
        if i > 0:
            gram[i - 1, j - 1] = s[k]
    for i in range(M - 1):
        gram[i, M - 1] = s[RHS + 1 + i] - s[PREV + 1 + i]
    gram[M - 1, M - 1] = s[NORM]
    row = gathered(rows)
    gamma = solve(gram, [entry(row, k) for k in range(M)], entries)
    gamma = [jnp.broadcast_to(g, (8, 128)) for g in gamma]
    for c in range(3):
        for p in range(value.shape[1]):
            tile = value[c, p]
            for j in range(M - 1):
                tile = tile - gamma[j] * hist[j + 1, c, p]
            field[c, p] = tile - gamma[M - 1] * (first_value[c, p] - prev[c, p])


def swap(cells, axes, start):
    pairs = [(i, i + 1) for i in range(start, lax.axis_size(axes) - 1, 2)]
    return lax.ppermute(cells, axes, pairs + [(j, i) for i, j in pairs])


def faces_of(even_pair, odd_pair):
    odd_pair = swap(odd_pair, GX, 1)
    return lax.all_gather(even_pair, GX[2]), odd_pair


def edges_of(even_pair, odd_pair):
    even_pair = swap(even_pair, GY, 0)
    odd_pair = swap(odd_pair, GY, 1)
    return even_pair, odd_pair


def exchange(payload):
    rows = lax.all_to_all(payload, CHAIN, 0, 0)
    row = jnp.sum(rows, axis=(0, 1))
    rows = jnp.broadcast_to(row[None, None, :], (lax.axis_size(PLANE), 1, 128))
    return lax.all_to_all(rows, PLANE, 0, 0)


def local(velocity, forcing, viscosity, residual_prev, value_prev, hist_res, hist_val):
    shape = velocity.shape
    entries = 1.0 * velocity.size * lax.axis_size(GX) * lax.axis_size(GY)
    fan = (lax.axis_size(CHAIN), 1, 128)
    work = ((8, 9, ROWS, 128), (8, 3, ROWS, 128), (8, 3, ROWS, 128))
    frames = (10 * FIELD * ROWS, 128)
    fixed = (8 * STATIC * ROWS, 128)

    hbm = [pl.BlockSpec(memory_space=pltpu.HBM)] * 4
    far_away = [pltpu.with_memory_space_constraint(x, pltpu.HBM) for x in (velocity, forcing, viscosity, hist_val)]
    *packed, velocity, forcing, viscosity = call(
        pack_first,
        [(17 + 9 * M, 8, 128), (17, 8, 128), shape, shape, shape[1:]],
        [pltpu.SemaphoreType.DMA((17 + 3 * M,))],
        in_specs=hbm,
    )(*far_away)
    faces = faces_of(*packed)
    (gram,) = call(gram_part, [(1, 128)], flops=4000000)(hist_res, residual_prev)
    edge = (edge_rows(True)[1], 128)
    packed = call(pack_second, [edge, edge], [(10 * FIELD * 8, 128), (8 * STATIC * 8, 128)])(
        velocity, forcing, viscosity, *faces
    )
    edges = edges_of(*packed)
    (far_hist,) = call(lambda field, out: pack_faces(field, None, out), [(9 * M, 8, 128)])(hist_val)
    far_hist = swap(far_hist, GX, 1)
    value, newest, static, payload = call(first_map, [shape, shape, fixed, fan], [frames, *work])(
        velocity, forcing, viscosity, *faces, *edges, hist_res, residual_prev, gram
    )
    sums = exchange(payload)
    packed = call(pack_faces, [(9, 8, 128)] * 2)(value)
    near_value, far_value = faces_of(*packed)
    near = (faces[0], near_value, far_value, far_hist)
    edge = (GROUPS * GROUP_ROWS, 128)
    packed = call(pack_mixed_second, [edge, edge], [(GROUPS, 10 * FIELD * 8, 128)])(value, hist_val, *near)
    edges = edges_of(*packed)
    value_next, resid, payload = call(
        lambda *refs: second_map(entries, *refs), [shape, shape, fan], [frames, (2, GROUP_ROWS, 128), *work]
    )(sums, value, hist_val, *near, *edges, static, hist_res, newest)
    next_sums = exchange(payload)
    return call(lambda *refs: mix_second(entries, *refs), [shape, shape])(
        next_sums, sums, value_next, hist_val, value, value_prev, resid
    )


def build(torus):
    in_specs = (
        P(None, GX, GY, None),
        P(None, GX, GY, None),
        P(GX, GY, None),
        P(None, GX, GY, None),
        P(None, GX, GY, None),
        P(None, None, GX, GY, None),
        P(None, None, GX, GY, None),
    )
    out_specs = (P(None, GX, GY, None), P(None, GX, GY, None))
    return jax.shard_map(local, mesh=torus, in_specs=in_specs, out_specs=out_specs, check_vma=False)


def solution(mesh):
    torus = Mesh(mesh.devices.reshape(2, 16, 2, 2, 8), AXES)
    return build(torus)
```

```python
import jax
import jax.numpy as jnp
from jax import lax
from jax.experimental import pallas as pl
from jax.experimental.pallas import tpu as pltpu
from jax.sharding import Mesh
from jax.sharding import PartitionSpec as P

M = 5
AXES = ("gx_0", "gx_1", "gx_2", "gy_0", "gy_1")
GX = ("gx_0", "gx_1", "gx_2")
GY = ("gy_0", "gy_1")
CHAIN = ("gx_1", "gx_2")
PLANE = ("gx_0", "gy_0", "gy_1")

REG = 0.05
FLOOR = 0.001
PAIRS = [(i, j) for i in range(M) for j in range(i, M)]
RHS = len(PAIRS)
PREV = RHS + M
NORM = PREV + M

ROWS = 16
OWN = 3
FIELD = 3
STATIC = 4


GROUPS = 1 + M
GROUP_ROWS = 56


def edge_rows(with_static):
    if with_static:
        return [(1, 3, 24, 0, False), (1, 4, 24, 24, True), (2, 8, 16, 48, True), (2, 6, 18, 64, False), (3, 9, 12, 88, False)], 104
    return [(1, 3, 24, 0, False), (2, 6, 18, 24, False), (3, 9, 12, 42, False)], GROUP_ROWS


def call(kernel, outs, scratch=(), flops=20000, **more):
    return pl.pallas_call(
        kernel,
        out_shape=[jax.ShapeDtypeStruct(s, jnp.float32) for s in outs],
        scratch_shapes=[pltpu.VMEM(s, jnp.float32) if isinstance(s, tuple) else s for s in scratch],
        compiler_params=pltpu.CompilerParams(vmem_limit_bytes=8 * 1024 * 1024),
        cost_estimate=pl.CostEstimate(flops=flops, bytes_accessed=100000, transcendentals=0),
        **more,
    )


def odd_place(axes):
    return lax.rem(lax.axis_index(axes[-1]), 2) == 1


def pack_first(vel, forcing, visc, hist, even_pair, odd_pair, vel_near, forcing_near, visc_near, sem):
    cx = vel.shape[1]
    odd = odd_place(GX)
    copies = []
    for out, low in ((even_pair, odd), (odd_pair, jnp.logical_not(odd))):
        three = pl.ds(jnp.where(low, 0, cx - 3), 3)
        two = pl.ds(jnp.where(low, 0, cx - 2), 2)
        pieces = [(vel.at[c, three], out.at[pl.ds(3 * c, 3)]) for c in range(3)]
        pieces += [(forcing.at[c, two], out.at[pl.ds(9 + 2 * c, 2)]) for c in range(3)]
        pieces += [(visc.at[two], out.at[pl.ds(15, 2)])]
        if out is even_pair:
            pieces += [(hist.at[j, c, three], out.at[pl.ds(17 + 9 * j + 3 * c, 3)]) for j in range(M) for c in range(3)]
        for src, dst in pieces:
            copies.append(pltpu.make_async_copy(src, dst, sem.at[len(copies)]))
            copies[-1].start()
    for src, dst in ((vel, vel_near), (forcing, forcing_near), (visc, visc_near)):
        copies.append(pltpu.make_async_copy(src, dst, sem.at[len(copies)]))
        copies[-1].start()
    for copy in copies:
        copy.wait()


def arrived(axes, even_pair, odd_pair):
    odd = odd_place(axes)
    if even_pair.shape != odd_pair.shape:
        even_pair = even_pair.at[jnp.where(odd, 0, 1)]
    before = lambda i: jnp.where(odd, even_pair[i], odd_pair[i])
    after = lambda i: jnp.where(odd, odd_pair[i], even_pair[i])
    return before, after


def field_tile(vel, left, right, tile):
    plane, c = divmod(tile, FIELD)
    cx = vel.shape[1]
    if plane < 3:
        return left(3 * c + plane)
    if plane < 3 + cx:
        return vel[c, plane - 3]
    return right(3 * c + plane - 3 - cx)


def static_tile(forcing, visc, left, right, tile):
    plane, c = divmod(tile, STATIC)
    cx = visc.shape[0]
    if plane < 2:
        return left(9 + 2 * c + plane)
    if plane < 2 + cx:
        return forcing[c, plane - 2] if c < 3 else visc[plane - 2]
    return right(9 + 2 * c + plane - 2 - cx)


def pack_edges(tiles, fixed, even_pair, odd_pair, base, with_static):
    odd = odd_place(GY)
    pieces, _ = edge_rows(with_static)
    for dist, first, count, row, static in pieces:
        src = fixed if static else tiles
        up = src[pl.ds(first * 8 + 8 - dist, count, stride=8), :]
        down = src[pl.ds(first * 8 + dist - 1, count, stride=8), :]
        even_pair[base + row : base + row + count] = jnp.where(odd, down, up)
        odd_pair[base + row : base + row + count] = jnp.where(odd, up, down)


def pack_second(vel, forcing, visc, near, far, even_pair, odd_pair, tiles, fixed):
    left, right = arrived(GX, near, far)
    for t in range(8 * STATIC):
        fixed[t * 8 : t * 8 + 8] = static_tile(forcing, visc, left, right, t)
    for t in range(10 * FIELD):
        tiles[t * 8 : t * 8 + 8] = field_tile(vel, left, right, t)
    pack_edges(tiles, fixed, even_pair, odd_pair, 0, True)


def pack_faces(field, even_pair, odd_pair):
    cx = field.shape[-3]
    odd = odd_place(GX)
    for out, low in ((even_pair, odd), (odd_pair, jnp.logical_not(odd))):
        if out is not None:
            first = jnp.where(low, 0, cx - 3)
            for g in range(out.shape[0] // 9):
                src = field.at[g] if len(field.shape) == 5 else field
                for c in range(3):
                    for d in range(3):
                        out[9 * g + 3 * c + d] = src[c, first + d]


def mixed_sides(near, near_value, far_value, far_hist):
    odd = odd_place(GX)
    near = near.at[jnp.where(odd, 0, 1)]
    near_value = near_value.at[jnp.where(odd, 0, 1)]
    even_pair = lambda i: near_value[i] if i < 9 else near[17 + i - 9]
    odd_pair = lambda i: far_value[i] if i < 9 else far_hist[i - 9]
    before = lambda i: jnp.where(odd, even_pair(i), odd_pair(i))
    after = lambda i: jnp.where(odd, odd_pair(i), even_pair(i))
    return before, after


def pack_mixed_second(value, hist, near, near_value, far_value, far_hist, even_pair, odd_pair, tiles):
    left, right = mixed_sides(near, near_value, far_value, far_hist)
    for g in range(GROUPS):
        src = value if g == 0 else hist.at[g - 1]
        block = tiles.at[g]
        for t in range(10 * FIELD):
            block[t * 8 : t * 8 + 8] = field_tile(src, lambda i: left(9 * g + i), lambda i: right(9 * g + i), t)
        pack_edges(block, None, even_pair, odd_pair, g * GROUP_ROWS, False)


def fill_frames(with_static, south, north, frames, fixed):
    pieces, _ = edge_rows(with_static)
    for dist, first, count, row, static in pieces:
        dst = fixed if static else frames
        dst[pl.ds(first * ROWS + OWN - dist, count, stride=ROWS), :] = south(row, count)
        dst[pl.ds(first * ROWS + OWN + 7 + dist, count, stride=ROWS), :] = north(row, count)


def sweeps(frames, fixed, coef, one, two):
    lane = lax.broadcasted_iota(jnp.int32, (ROWS, 128), 1)
    field = lambda p, c: frames[(p * FIELD + c) * ROWS : (p * FIELD + c + 1) * ROWS]
    still = lambda s, c: fixed[(s * STATIC + c) * ROWS : (s * STATIC + c + 1) * ROWS]
    for s in range(8):
        a = [field(s + 1, c) for c in range(3)]
        visc = still(s, 3)
        inv = 1.0 / (1.0 + 6.0 * visc + jnp.abs(a[0]) + jnp.abs(a[1]) + jnp.abs(a[2]))
        for k in range(3):
            low = (visc + jnp.maximum(a[k], 0.0)) * inv
            high = (visc - jnp.minimum(a[k], 0.0)) * inv
            if k == 2:
                low = jnp.where(lane > 0, low, 0.0)
                high = jnp.where(lane < 127, high, 0.0)
            coef[s, 2 * k] = low
            coef[s, 2 * k + 1] = high
            coef[s, 6 + k] = (still(s, k) + a[k]) * inv

    def relax(src, s, c):
        mid = src(0)
        total = coef[s, 6 + c] + coef[s, 0] * src(-1) + coef[s, 1] * src(1)
        total = total + coef[s, 2] * pltpu.roll(mid, 1, 0) + coef[s, 3] * pltpu.roll(mid, ROWS - 1, 0)
        return total + coef[s, 4] * pltpu.roll(mid, 1, 1) + coef[s, 5] * pltpu.roll(mid, 127, 1)

    for s in range(8):
        for c in range(3):
            one[s, c] = relax(lambda d: field(s + 1 + d, c), s, c)
    for s in range(1, 7):
        for c in range(3):
            two[s, c] = relax(lambda d: one[s + d, c], s, c)
    out = {}
    for s in range(2, 6):
        for c in range(3):
            out[c, s - 2] = relax(lambda d: two[s + d, c], s, c)[OWN : OWN + 8]
    return out


def lanes(shape=(1, 128)):
    return lax.broadcasted_iota(jnp.int32, shape, 1)


def spread(row, parts):
    lane = lanes()
    for k, part in parts.items():
        whole = jnp.sum(jnp.sum(part, axis=0, keepdims=True), axis=1, keepdims=True)
        row = jnp.where(lane == k, whole, row)
    return row


def gram_part(hist, prev, out):
    tiles = [(c, p) for c in range(3) for p in range(hist.shape[2])]
    parts = {}
    for k, (i, j) in enumerate(PAIRS):
        parts[k] = sum(hist[i, c, p] * hist[j, c, p] for c, p in tiles)
    for i in range(M):
        parts[PREV + i] = sum(hist[i, c, p] * prev[c, p] for c, p in tiles)
    out[...] = spread(jnp.zeros((1, 128), jnp.float32), parts)


def first_map(vel, forcing, visc, near, far, even_pair, odd_pair, hist, prev, gram, value, newest, fixed, even_faces, odd_faces, frames, coef, one, two):
    frames[...] = jnp.zeros_like(frames)
    fixed[...] = jnp.zeros_like(fixed)
    left, right = arrived(GX, near, far)
    for t in range(8 * STATIC):
        fixed[t * ROWS + OWN : t * ROWS + OWN + 8] = static_tile(forcing, visc, left, right, t)
    for t in range(10 * FIELD):
        frames[t * ROWS + OWN : t * ROWS + OWN + 8] = field_tile(vel, left, right, t)
    south, north = arrived(GY, even_pair, odd_pair)
    fill_frames(True, lambda r, n: south(pl.ds(r, n)), lambda r, n: north(pl.ds(r, n)), frames, fixed)
    result = sweeps(frames, fixed, coef, one, two)
    resid = {}
    fresh = {}
    for (c, p), tile in result.items():
        value[c, p] = tile
        resid[c, p] = tile - vel[c, p]
        fresh[c, p] = resid[c, p] - prev[c, p]
        newest[c, p] = fresh[c, p]
    parts = {RHS + i: sum(hist[i, c, p] * r for (c, p), r in resid.items()) for i in range(M)}
    parts[NORM] = sum(f * f for f in fresh.values())
    even_faces[9] = jnp.broadcast_to(spread(gram[...], parts), (8, 128))
    pack_faces(value, even_faces, odd_faces)


def chip_row(gathered_faces, payload):
    row = gathered_faces[0, 9, 0:1] + gathered_faces[1, 9, 0:1]
    for k in range(payload.shape[0]):
        payload[k] = row


def entry(row, k):
    return jnp.sum(jnp.where(lanes() == k, row, 0.0), axis=1, keepdims=True)


def solve(gram, rhs, entries):
    shift = (REG / M) * sum(gram[i, i] for i in range(M)) + FLOOR * entries
    a = {(i, j): gram[min(i, j), max(i, j)] for i in range(M) for j in range(M)}
    for i in range(M):
        a[i, i] = a[i, i] + shift
    r = list(rhs)
    inv = []
    for k in range(M):
        inv.append(1.0 / a[k, k])
        for i in range(k + 1, M):
            f = a[k, i] * inv[k]
            for j in range(i, M):
                a[i, j] = a[i, j] - f * a[k, j]
            r[i] = r[i] - f * r[k]
    out = [None] * M
    for i in reversed(range(M)):
        acc = r[i]
        for j in range(i + 1, M):
            acc = acc - a[i, j] * out[j]
        out[i] = acc * inv[i]
    return out


def gathered(rows):
    total = rows[0]
    for k in range(1, rows.shape[0]):
        total = total + rows[k]
    return total


def second_map(entries, rows, value, hist_val, near, near_value, far_value, far_hist, even_pair, odd_pair, fixed, hist, newest, value_next, resid, payload, frames, edges, coef, one, two):
    row = gathered(rows)
    s = [entry(row, k) for k in range(PREV)]
    gram = {pair: s[k] for k, pair in enumerate(PAIRS)}
    gamma = [jnp.broadcast_to(g, (8, 128)) for g in solve(gram, s[RHS:PREV], entries)]

    def mixed(part):
        total = part(0)
        for j in range(M):
            total = total - gamma[j] * part(j + 1)
        return total

    frames[...] = jnp.zeros_like(frames)
    left, right = mixed_sides(near, near_value, far_value, far_hist)
    field = {}
    for t in range(10 * FIELD):
        plane, c = divmod(t, FIELD)
        tile = mixed(
            lambda g: field_tile(value if g == 0 else hist_val.at[g - 1], lambda i: left(9 * g + i), lambda i: right(9 * g + i), t)
        )
        frames[t * ROWS + OWN : t * ROWS + OWN + 8] = tile
        if 3 <= plane < 7:
            field[c, plane - 3] = tile
    south, north = arrived(GY, even_pair, odd_pair)
    for side, reader in enumerate((south, north)):
        for r in range(0, GROUP_ROWS, 8):
            edges[side, r : r + 8] = mixed(lambda g: reader(pl.ds(g * GROUP_ROWS + r, 8)))
    fill_frames(False, lambda r, n: edges[0, r : r + n], lambda r, n: edges[1, r : r + n], frames, None)
    result = sweeps(frames, fixed, coef, one, two)
    for (c, p), tile in result.items():
        value_next[c, p] = tile
        result[c, p] = tile - field[c, p]
        resid[c, p] = result[c, p]
    parts = {i: sum(hist[i + 1, c, p] * r for (c, p), r in result.items()) for i in range(M - 1)}
    parts[M - 1] = sum(newest[c, p] * r for (c, p), r in result.items())
    row = spread(jnp.zeros((1, 128), jnp.float32), parts)
    for k in range(payload.shape[0]):
        payload[k] = row


def mix_second(entries, rows, first_rows, value, hist, first_value, prev, resid, field, resid_out):
    resid_out[...] = resid[...]
    row = gathered(first_rows)
    s = [entry(row, k) for k in range(NORM + 1)]
    gram = {}
    for k, (i, j) in enumerate(PAIRS):
        if i > 0:
            gram[i - 1, j - 1] = s[k]
    for i in range(M - 1):
        gram[i, M - 1] = s[RHS + 1 + i] - s[PREV + 1 + i]
    gram[M - 1, M - 1] = s[NORM]
    row = gathered(rows)
    gamma = solve(gram, [entry(row, k) for k in range(M)], entries)
    gamma = [jnp.broadcast_to(g, (8, 128)) for g in gamma]
    for c in range(3):
        for p in range(value.shape[1]):
            tile = value[c, p]
            for j in range(M - 1):
                tile = tile - gamma[j] * hist[j + 1, c, p]
            field[c, p] = tile - gamma[M - 1] * (first_value[c, p] - prev[c, p])


def swap(cells, axes, start):
    pairs = [(i, i + 1) for i in range(start, lax.axis_size(axes) - 1, 2)]
    return lax.ppermute(cells, axes, pairs + [(j, i) for i, j in pairs])


def faces_of(even_pair, odd_pair):
    odd_pair = swap(odd_pair, GX, 1)
    return lax.all_gather(even_pair, GX[2]), odd_pair


def edges_of(even_pair, odd_pair):
    even_pair = swap(even_pair, GY, 0)
    odd_pair = swap(odd_pair, GY, 1)
    return even_pair, odd_pair


def exchange(payload, group):
    rows = lax.all_to_all(payload, group, 0, 0)
    row = jnp.sum(rows, axis=(0, 1))
    rows = jnp.broadcast_to(row[None, None, :], (lax.axis_size(PLANE), 1, 128))
    return lax.all_to_all(rows, PLANE, 0, 0)


def local(velocity, forcing, viscosity, residual_prev, value_prev, hist_res, hist_val):
    shape = velocity.shape
    entries = 1.0 * velocity.size * lax.axis_size(GX) * lax.axis_size(GY)
    fan = (lax.axis_size(CHAIN), 1, 128)
    work = ((8, 9, ROWS, 128), (8, 3, ROWS, 128), (8, 3, ROWS, 128))
    frames = (10 * FIELD * ROWS, 128)
    fixed = (8 * STATIC * ROWS, 128)

    hbm = [pl.BlockSpec(memory_space=pltpu.HBM)] * 4
    far_away = [pltpu.with_memory_space_constraint(x, pltpu.HBM) for x in (velocity, forcing, viscosity, hist_val)]
    *packed, velocity, forcing, viscosity = call(
        pack_first,
        [(17 + 9 * M, 8, 128), (17, 8, 128), shape, shape, shape[1:]],
        [pltpu.SemaphoreType.DMA((17 + 3 * M,))],
        in_specs=hbm,
    )(*far_away)
    faces = faces_of(*packed)
    (gram,) = call(gram_part, [(1, 128)], flops=4000000)(hist_res, residual_prev)
    edge = (edge_rows(True)[1], 128)
    packed = call(pack_second, [edge, edge], [(10 * FIELD * 8, 128), (8 * STATIC * 8, 128)])(
        velocity, forcing, viscosity, *faces
    )
    edges = edges_of(*packed)
    (far_hist,) = call(lambda field, out: pack_faces(field, None, out), [(9 * M, 8, 128)])(hist_val)
    far_hist = swap(far_hist, GX, 1)
    value, newest, static, even_faces, odd_faces = call(
        first_map, [shape, shape, fixed, (10, 8, 128), (9, 8, 128)], [frames, *work]
    )(velocity, forcing, viscosity, *faces, *edges, hist_res, residual_prev, gram)
    near_value = lax.all_gather(even_faces, GX[2])
    (payload,) = call(chip_row, [(lax.axis_size(GX[1]), 1, 128)])(near_value)
    sums = exchange(payload, GX[1])
    far_value = swap(odd_faces, GX, 1)
    near = (faces[0], near_value, far_value, far_hist)
    edge = (GROUPS * GROUP_ROWS, 128)
    packed = call(pack_mixed_second, [edge, edge], [(GROUPS, 10 * FIELD * 8, 128)])(value, hist_val, *near)
    edges = edges_of(*packed)
    value_next, resid, payload = call(
        lambda *refs: second_map(entries, *refs), [shape, shape, fan], [frames, (2, GROUP_ROWS, 128), *work]
    )(sums, value, hist_val, *near, *edges, static, hist_res, newest)
    next_sums = exchange(payload, CHAIN)
    return call(lambda *refs: mix_second(entries, *refs), [shape, shape])(
        next_sums, sums, value_next, hist_val, value, value_prev, resid
    )


def build(torus):
    in_specs = (
        P(None, GX, GY, None),
        P(None, GX, GY, None),
        P(GX, GY, None),
        P(None, GX, GY, None),
        P(None, GX, GY, None),
        P(None, None, GX, GY, None),
        P(None, None, GX, GY, None),
    )
    out_specs = (P(None, GX, GY, None), P(None, GX, GY, None))
    return jax.shard_map(local, mesh=torus, in_specs=in_specs, out_specs=out_specs, check_vma=False)


def solution(mesh):
    torus = Mesh(mesh.devices.reshape(2, 16, 2, 2, 8), AXES)
    return build(torus)
```

```python
import jax
import jax.numpy as jnp
from jax import lax
from jax.experimental import pallas as pl
from jax.experimental.pallas import tpu as pltpu
from jax.sharding import Mesh
from jax.sharding import PartitionSpec as P

M = 5
AXES = ("gx_0", "gx_1", "gx_2", "gy_0", "gy_1")
GX = ("gx_0", "gx_1", "gx_2")
GY = ("gy_0", "gy_1")
CHAIN = ("gx_1", "gx_2")
PLANE = ("gx_0", "gy_0", "gy_1")

REG = 0.05
FLOOR = 0.001
PAIRS = [(i, j) for i in range(M) for j in range(i, M)]
RHS = len(PAIRS)
PREV = RHS + M
NORM = PREV + M

ROWS = 16
OWN = 3
FIELD = 3
STATIC = 4


GROUPS = 1 + M
GROUP_ROWS = 56


def edge_rows(with_static):
    if with_static:
        return [(1, 3, 24, 0, False), (1, 4, 24, 24, True), (2, 8, 16, 48, True), (2, 6, 18, 64, False), (3, 9, 12, 88, False)], 104
    return [(1, 3, 24, 0, False), (2, 6, 18, 24, False), (3, 9, 12, 42, False)], GROUP_ROWS


def call(kernel, outs, scratch=(), flops=20000, **more):
    return pl.pallas_call(
        kernel,
        out_shape=[jax.ShapeDtypeStruct(s, jnp.float32) for s in outs],
        scratch_shapes=[pltpu.VMEM(s, jnp.float32) if isinstance(s, tuple) else s for s in scratch],
        compiler_params=pltpu.CompilerParams(vmem_limit_bytes=8 * 1024 * 1024),
        cost_estimate=pl.CostEstimate(flops=flops, bytes_accessed=100000, transcendentals=0),
        **more,
    )


def odd_place(axes):
    return lax.rem(lax.axis_index(axes[-1]), 2) == 1


def pack_first(vel, forcing, visc, hist, even_pair, odd_pair, vel_near, forcing_near, visc_near, sem):
    cx = vel.shape[1]
    odd = odd_place(GX)
    copies = []
    for out, low in ((even_pair, odd), (odd_pair, jnp.logical_not(odd))):
        three = pl.ds(jnp.where(low, 0, cx - 3), 3)
        two = pl.ds(jnp.where(low, 0, cx - 2), 2)
        pieces = [(vel.at[c, three], out.at[pl.ds(3 * c, 3)]) for c in range(3)]
        pieces += [(forcing.at[c, two], out.at[pl.ds(9 + 2 * c, 2)]) for c in range(3)]
        pieces += [(visc.at[two], out.at[pl.ds(15, 2)])]
        if out is even_pair:
            pieces += [(hist.at[j, c, three], out.at[pl.ds(17 + 9 * j + 3 * c, 3)]) for j in range(M) for c in range(3)]
        for src, dst in pieces:
            copies.append(pltpu.make_async_copy(src, dst, sem.at[len(copies)]))
            copies[-1].start()
    for src, dst in ((vel, vel_near), (forcing, forcing_near), (visc, visc_near)):
        copies.append(pltpu.make_async_copy(src, dst, sem.at[len(copies)]))
        copies[-1].start()
    for copy in copies:
        copy.wait()


def arrived(axes, even_pair, odd_pair):
    odd = odd_place(axes)
    if even_pair.shape != odd_pair.shape:
        even_pair = even_pair.at[jnp.where(odd, 0, 1)]
    before = lambda i: jnp.where(odd, even_pair[i], odd_pair[i])
    after = lambda i: jnp.where(odd, odd_pair[i], even_pair[i])
    return before, after


def field_tile(vel, left, right, tile):
    plane, c = divmod(tile, FIELD)
    cx = vel.shape[1]
    if plane < 3:
        return left(3 * c + plane)
    if plane < 3 + cx:
        return vel[c, plane - 3]
    return right(3 * c + plane - 3 - cx)


def static_tile(forcing, visc, left, right, tile):
    plane, c = divmod(tile, STATIC)
    cx = visc.shape[0]
    if plane < 2:
        return left(9 + 2 * c + plane)
    if plane < 2 + cx:
        return forcing[c, plane - 2] if c < 3 else visc[plane - 2]
    return right(9 + 2 * c + plane - 2 - cx)


def pack_edges(tiles, fixed, even_pair, odd_pair, base, with_static):
    odd = odd_place(GY)
    pieces, _ = edge_rows(with_static)
    for dist, first, count, row, static in pieces:
        src = fixed if static else tiles
        up = src[pl.ds(first * 8 + 8 - dist, count, stride=8), :]
        down = src[pl.ds(first * 8 + dist - 1, count, stride=8), :]
        even_pair[base + row : base + row + count] = jnp.where(odd, down, up)
        odd_pair[base + row : base + row + count] = jnp.where(odd, up, down)


def pack_second(vel, forcing, visc, near, far, even_pair, odd_pair, tiles, fixed):
    left, right = arrived(GX, near, far)
    for t in range(8 * STATIC):
        fixed[t * 8 : t * 8 + 8] = static_tile(forcing, visc, left, right, t)
    for t in range(10 * FIELD):
        tiles[t * 8 : t * 8 + 8] = field_tile(vel, left, right, t)
    pack_edges(tiles, fixed, even_pair, odd_pair, 0, True)


def pack_faces(field, even_pair, odd_pair):
    cx = field.shape[-3]
    odd = odd_place(GX)
    for out, low in ((even_pair, odd), (odd_pair, jnp.logical_not(odd))):
        if out is not None:
            first = jnp.where(low, 0, cx - 3)
            for g in range(out.shape[0] // 9):
                src = field.at[g] if len(field.shape) == 5 else field
                for c in range(3):
                    for d in range(3):
                        out[9 * g + 3 * c + d] = src[c, first + d]


def mixed_sides(near, near_value, far_value, far_hist):
    odd = odd_place(GX)
    near = near.at[jnp.where(odd, 0, 1)]
    near_value = near_value.at[jnp.where(odd, 0, 1)]
    even_pair = lambda i: near_value[i] if i < 9 else near[17 + i - 9]
    odd_pair = lambda i: far_value[i] if i < 9 else far_hist[i - 9]
    before = lambda i: jnp.where(odd, even_pair(i), odd_pair(i))
    after = lambda i: jnp.where(odd, odd_pair(i), even_pair(i))
    return before, after


def pack_mixed_second(value, hist, near, near_value, far_value, far_hist, even_pair, odd_pair, tiles):
    left, right = mixed_sides(near, near_value, far_value, far_hist)
    for g in range(GROUPS):
        src = value if g == 0 else hist.at[g - 1]
        block = tiles.at[g]
        for t in range(10 * FIELD):
            block[t * 8 : t * 8 + 8] = field_tile(src, lambda i: left(9 * g + i), lambda i: right(9 * g + i), t)
        pack_edges(block, None, even_pair, odd_pair, g * GROUP_ROWS, False)


def fill_frames(with_static, south, north, frames, fixed):
    pieces, _ = edge_rows(with_static)
    for dist, first, count, row, static in pieces:
        dst = fixed if static else frames
        dst[pl.ds(first * ROWS + OWN - dist, count, stride=ROWS), :] = south(row, count)
        dst[pl.ds(first * ROWS + OWN + 7 + dist, count, stride=ROWS), :] = north(row, count)


def sweeps(frames, fixed, coef, one, two):
    lane = lax.broadcasted_iota(jnp.int32, (ROWS, 128), 1)
    field = lambda p, c: frames[(p * FIELD + c) * ROWS : (p * FIELD + c + 1) * ROWS]
    still = lambda s, c: fixed[(s * STATIC + c) * ROWS : (s * STATIC + c + 1) * ROWS]
    for s in range(8):
        a = [field(s + 1, c) for c in range(3)]
        visc = still(s, 3)
        inv = 1.0 / (1.0 + 6.0 * visc + jnp.abs(a[0]) + jnp.abs(a[1]) + jnp.abs(a[2]))
        for k in range(3):
            low = (visc + jnp.maximum(a[k], 0.0)) * inv
            high = (visc - jnp.minimum(a[k], 0.0)) * inv
            if k == 2:
                low = jnp.where(lane > 0, low, 0.0)
                high = jnp.where(lane < 127, high, 0.0)
            coef[s, 2 * k] = low
            coef[s, 2 * k + 1] = high
            coef[s, 6 + k] = (still(s, k) + a[k]) * inv

    def relax(src, s, c):
        mid = src(0)
        total = coef[s, 6 + c] + coef[s, 0] * src(-1) + coef[s, 1] * src(1)
        total = total + coef[s, 2] * pltpu.roll(mid, 1, 0) + coef[s, 3] * pltpu.roll(mid, ROWS - 1, 0)
        return total + coef[s, 4] * pltpu.roll(mid, 1, 1) + coef[s, 5] * pltpu.roll(mid, 127, 1)

    for s in range(8):
        for c in range(3):
            one[s, c] = relax(lambda d: field(s + 1 + d, c), s, c)
    for s in range(1, 7):
        for c in range(3):
            two[s, c] = relax(lambda d: one[s + d, c], s, c)
    out = {}
    for s in range(2, 6):
        for c in range(3):
            out[c, s - 2] = relax(lambda d: two[s + d, c], s, c)[OWN : OWN + 8]
    return out


def lanes(shape=(1, 128)):
    return lax.broadcasted_iota(jnp.int32, shape, 1)


def spread(row, parts):
    lane = lanes()
    for k, part in parts.items():
        whole = jnp.sum(jnp.sum(part, axis=0, keepdims=True), axis=1, keepdims=True)
        row = jnp.where(lane == k, whole, row)
    return row


def gram_part(hist, prev, out):
    tiles = [(c, p) for c in range(3) for p in range(hist.shape[2])]
    parts = {}
    for k, (i, j) in enumerate(PAIRS):
        parts[k] = sum(hist[i, c, p] * hist[j, c, p] for c, p in tiles)
    for i in range(M):
        parts[PREV + i] = sum(hist[i, c, p] * prev[c, p] for c, p in tiles)
    out[...] = spread(jnp.zeros((1, 128), jnp.float32), parts)


def first_map(vel, forcing, visc, near, far, even_pair, odd_pair, hist, prev, gram, value, newest, fixed, payload, frames, coef, one, two):
    frames[...] = jnp.zeros_like(frames)
    fixed[...] = jnp.zeros_like(fixed)
    left, right = arrived(GX, near, far)
    for t in range(8 * STATIC):
        fixed[t * ROWS + OWN : t * ROWS + OWN + 8] = static_tile(forcing, visc, left, right, t)
    for t in range(10 * FIELD):
        frames[t * ROWS + OWN : t * ROWS + OWN + 8] = field_tile(vel, left, right, t)
    south, north = arrived(GY, even_pair, odd_pair)
    fill_frames(True, lambda r, n: south(pl.ds(r, n)), lambda r, n: north(pl.ds(r, n)), frames, fixed)
    result = sweeps(frames, fixed, coef, one, two)
    resid = {}
    fresh = {}
    for (c, p), tile in result.items():
        value[c, p] = tile
        resid[c, p] = tile - vel[c, p]
        fresh[c, p] = resid[c, p] - prev[c, p]
        newest[c, p] = fresh[c, p]
    parts = {RHS + i: sum(hist[i, c, p] * r for (c, p), r in resid.items()) for i in range(M)}
    parts[NORM] = sum(f * f for f in fresh.values())
    row = spread(gram[...], parts)
    for k in range(payload.shape[0]):
        payload[k] = row


def entry(row, k):
    return jnp.sum(jnp.where(lanes() == k, row, 0.0), axis=1, keepdims=True)


def solve(gram, rhs, entries):
    shift = (REG / M) * sum(gram[i, i] for i in range(M)) + FLOOR * entries
    a = {(i, j): gram[min(i, j), max(i, j)] for i in range(M) for j in range(M)}
    for i in range(M):
        a[i, i] = a[i, i] + shift
    r = list(rhs)
    inv = []
    for k in range(M):
        inv.append(1.0 / a[k, k])
        for i in range(k + 1, M):
            f = a[k, i] * inv[k]
            for j in range(i, M):
                a[i, j] = a[i, j] - f * a[k, j]
            r[i] = r[i] - f * r[k]
    out = [None] * M
    for i in reversed(range(M)):
        acc = r[i]
        for j in range(i + 1, M):
            acc = acc - a[i, j] * out[j]
        out[i] = acc * inv[i]
    return out


def gathered(rows):
    total = rows[0]
    for k in range(1, rows.shape[0]):
        total = total + rows[k]
    return total


def second_map(entries, rows, value, hist_val, near, near_value, far_value, far_hist, even_pair, odd_pair, fixed, hist, newest, value_next, resid, payload, frames, edges, coef, one, two):
    row = gathered(rows)
    s = [entry(row, k) for k in range(PREV)]
    gram = {pair: s[k] for k, pair in enumerate(PAIRS)}
    gamma = [jnp.broadcast_to(g, (8, 128)) for g in solve(gram, s[RHS:PREV], entries)]

    def mixed(part):
        total = part(0)
        for j in range(M):
            total = total - gamma[j] * part(j + 1)
        return total

    frames[...] = jnp.zeros_like(frames)
    left, right = mixed_sides(near, near_value, far_value, far_hist)
    field = {}
    for t in range(10 * FIELD):
        plane, c = divmod(t, FIELD)
        tile = mixed(
            lambda g: field_tile(value if g == 0 else hist_val.at[g - 1], lambda i: left(9 * g + i), lambda i: right(9 * g + i), t)
        )
        frames[t * ROWS + OWN : t * ROWS + OWN + 8] = tile
        if 3 <= plane < 7:
            field[c, plane - 3] = tile
    south, north = arrived(GY, even_pair, odd_pair)
    for side, reader in enumerate((south, north)):
        for r in range(0, GROUP_ROWS, 8):
            edges[side, r : r + 8] = mixed(lambda g: reader(pl.ds(g * GROUP_ROWS + r, 8)))
    fill_frames(False, lambda r, n: edges[0, r : r + n], lambda r, n: edges[1, r : r + n], frames, None)
    result = sweeps(frames, fixed, coef, one, two)
    for (c, p), tile in result.items():
        value_next[c, p] = tile
        result[c, p] = tile - field[c, p]
        resid[c, p] = result[c, p]
    parts = {i: sum(hist[i + 1, c, p] * r for (c, p), r in result.items()) for i in range(M - 1)}
    parts[M - 1] = sum(newest[c, p] * r for (c, p), r in result.items())
    row = spread(jnp.zeros((1, 128), jnp.float32), parts)
    for k in range(payload.shape[0]):
        payload[k] = row


def mix_second(entries, rows, first_rows, value, hist, first_value, prev, resid, field, resid_out):
    resid_out[...] = resid[...]
    row = gathered(first_rows)
    s = [entry(row, k) for k in range(NORM + 1)]
    gram = {}
    for k, (i, j) in enumerate(PAIRS):
        if i > 0:
            gram[i - 1, j - 1] = s[k]
    for i in range(M - 1):
        gram[i, M - 1] = s[RHS + 1 + i] - s[PREV + 1 + i]
    gram[M - 1, M - 1] = s[NORM]
    row = gathered(rows)
    gamma = solve(gram, [entry(row, k) for k in range(M)], entries)
    gamma = [jnp.broadcast_to(g, (8, 128)) for g in gamma]
    for c in range(3):
        for p in range(value.shape[1]):
            tile = value[c, p]
            for j in range(M - 1):
                tile = tile - gamma[j] * hist[j + 1, c, p]
            field[c, p] = tile - gamma[M - 1] * (first_value[c, p] - prev[c, p])


def swap(cells, axes, start):
    pairs = [(i, i + 1) for i in range(start, lax.axis_size(axes) - 1, 2)]
    return lax.ppermute(cells, axes, pairs + [(j, i) for i, j in pairs])


def faces_of(even_pair, odd_pair):
    odd_pair = swap(odd_pair, GX, 1)
    return lax.all_gather(even_pair, GX[2]), odd_pair


def edges_of(even_pair, odd_pair):
    even_pair = swap(even_pair, GY, 0)
    odd_pair = swap(odd_pair, GY, 1)
    return even_pair, odd_pair


def exchange(payload, first, second):
    rows = lax.all_to_all(payload, first, 0, 0)
    row = jnp.sum(rows, axis=(0, 1))
    rows = jnp.broadcast_to(row[None, None, :], (lax.axis_size(second), 1, 128))
    return lax.all_to_all(rows, second, 0, 0)


def local(velocity, forcing, viscosity, residual_prev, value_prev, hist_res, hist_val):
    shape = velocity.shape
    entries = 1.0 * velocity.size * lax.axis_size(GX) * lax.axis_size(GY)
    fan = (lax.axis_size(CHAIN), 1, 128)
    work = ((8, 9, ROWS, 128), (8, 3, ROWS, 128), (8, 3, ROWS, 128))
    frames = (10 * FIELD * ROWS, 128)
    fixed = (8 * STATIC * ROWS, 128)

    hbm = [pl.BlockSpec(memory_space=pltpu.HBM)] * 4
    far_away = [pltpu.with_memory_space_constraint(x, pltpu.HBM) for x in (velocity, forcing, viscosity, hist_val)]
    *packed, velocity, forcing, viscosity = call(
        pack_first,
        [(17 + 9 * M, 8, 128), (17, 8, 128), shape, shape, shape[1:]],
        [pltpu.SemaphoreType.DMA((17 + 3 * M,))],
        in_specs=hbm,
    )(*far_away)
    faces = faces_of(*packed)
    (gram,) = call(gram_part, [(1, 128)], flops=4000000)(hist_res, residual_prev)
    edge = (edge_rows(True)[1], 128)
    packed = call(pack_second, [edge, edge], [(10 * FIELD * 8, 128), (8 * STATIC * 8, 128)])(
        velocity, forcing, viscosity, *faces
    )
    edges = edges_of(*packed)
    (far_hist,) = call(lambda field, out: pack_faces(field, None, out), [(9 * M, 8, 128)])(hist_val)
    far_hist = swap(far_hist, GX, 1)
    value, newest, static, payload = call(first_map, [shape, shape, fixed, fan], [frames, *work])(
        velocity, forcing, viscosity, *faces, *edges, hist_res, residual_prev, gram
    )
    sums = exchange(payload, CHAIN, PLANE)
    packed = call(pack_faces, [(9, 8, 128)] * 2)(value)
    near_value, far_value = faces_of(*packed)
    near = (faces[0], near_value, far_value, far_hist)
    edge = (GROUPS * GROUP_ROWS, 128)
    packed = call(pack_mixed_second, [edge, edge], [(GROUPS, 10 * FIELD * 8, 128)])(value, hist_val, *near)
    edges = edges_of(*packed)
    value_next, resid, payload = call(
        lambda *refs: second_map(entries, *refs), [shape, shape, (lax.axis_size(PLANE), 1, 128)], [frames, (2, GROUP_ROWS, 128), *work]
    )(sums, value, hist_val, *near, *edges, static, hist_res, newest)
    next_sums = exchange(payload, PLANE, CHAIN)
    return call(lambda *refs: mix_second(entries, *refs), [shape, shape])(
        next_sums, sums, value_next, hist_val, value, value_prev, resid
    )


def build(torus):
    in_specs = (
        P(None, GX, GY, None),
        P(None, GX, GY, None),
        P(GX, GY, None),
        P(None, GX, GY, None),
        P(None, GX, GY, None),
        P(None, None, GX, GY, None),
        P(None, None, GX, GY, None),
    )
    out_specs = (P(None, GX, GY, None), P(None, GX, GY, None))
    return jax.shard_map(local, mesh=torus, in_specs=in_specs, out_specs=out_specs, check_vma=False)


def solution(mesh):
    torus = Mesh(mesh.devices.reshape(2, 16, 2, 2, 8), AXES)
    return build(torus)
```
